128 devices in a mesh: batch: 8 (over x, core), rows: 16 (over z, y).
Axes of the slice: x: 4, y: 4, z: 4, core: 2. Of those that a mesh axis runs over, the one named last changes fastest.
Arguments:
- feat_quarter: bfloat16 [8, 256, 512, 256], P('batch', 'rows'), may hold values from -12 to 12
- feat_eighth: bfloat16 [8, 128, 256, 256], P('batch', 'rows'), may hold values from -12 to 12
- feat_sixteenth: bfloat16 [8, 64, 128, 256], P('batch', 'rows'), may hold values from -12 to 12
- feat_thirty: bfloat16 [8, 32, 64, 256], P('batch', 'rows'), may hold values from -12 to 12
- labels: int32 [8, 256, 512], P('batch', 'rows'), may hold values from 0 to 255, as said below
- first_weights: bfloat16 [4, 3, 3, 256, 128], replicated, may hold values from -0.125 to 0.125
- inner_weights: bfloat16 [3, 3, 3, 128, 128], replicated, may hold values from -0.1875 to 0.1875
- norm_gain: float32 [7, 128], replicated, may hold values from 0.1 to 1.9
- norm_shift: float32 [7, 128], replicated, may hold values from -3 to 3
- class_weight: bfloat16 [128, 19], replicated, may hold values from -0.5 to 0.5
- class_bias: float32 [19], replicated, may hold values from -3 to 3
Outputs:
- logits: bfloat16 [8, 19, 256, 512], P('batch', None, 'rows')
- mean_loss: float32 [], replicated
The draws below stay inside these ranges and needn't reach their ends.
Inputs may be any that keep to these rules, and one draw needn't show every extreme that they name: `labels`: values 0 to 18 name classes; 255 marks a pixel without a label.
All inputs are finite; a program needn't handle non-finite values.
Results may differ from the reference program's by a relative error of at most 0.008.
Values may be sent and summed in bfloat16 or wider, within the bound.
A program may use at most 128 MiB of HBM per device.

```python
import jax
import jax.numpy as jnp
from jax import lax

C_IN = 256
HEAD = 128
CLASSES = 19
GROUPS = 32
COLS4 = 512
IMAGES = 8
QUARTER_ROWS = 256


def feature_map(key, row_count, col_count, marker):
    level_key = jax.random.fold_in(key, marker)
    base_key, offset_key, slope_key = jax.random.split(level_key, 3)
    array_shape = (IMAGES, row_count, col_count, C_IN)
    row_ramp = ((jnp.arange(row_count, dtype=jnp.float32) + 0.5) / row_count)[None, :, None, None]
    base = jax.random.normal(base_key, array_shape, jnp.float32)
    slope_rate = jax.random.uniform(slope_key, (IMAGES, 1, 1, 1), jnp.float32, 1.0, 1.6)
    offset = jax.random.normal(offset_key, (IMAGES, 1, 1, C_IN), jnp.float32) * 0.5
    row_scale = jnp.exp(1.4 * slope_rate * (row_ramp - 0.5))
    values = base * row_scale + 2.0 * offset * row_ramp
    return jnp.clip(values, -12.0, 12.0).astype(jnp.bfloat16)


def draw_feat_quarter(key, part):
    return feature_map(key, QUARTER_ROWS, COLS4, 11)


def draw_feat_eighth(key, part):
    return feature_map(key, QUARTER_ROWS // 2, COLS4 // 2, 12)


def draw_feat_sixteenth(key, part):
    return feature_map(key, QUARTER_ROWS // 4, COLS4 // 4, 13)


def draw_feat_thirty(key, part):
    return feature_map(key, QUARTER_ROWS // 8, COLS4 // 8, 14)


def draw_labels(key, part):
    class_key, drop_key, major_key, choose_key = jax.random.split(jax.random.fold_in(key, 7), 4)
    array_shape = (IMAGES, QUARTER_ROWS, COLS4)
    classes = jax.random.randint(class_key, array_shape, 0, CLASSES)
    majors = jax.random.randint(major_key, (IMAGES, QUARTER_ROWS // 8), 0, CLASSES)
    row_index = jnp.arange(QUARTER_ROWS, dtype=jnp.int32)
    block_major = majors[:, row_index // 8][:, :, None]
    choose = jax.random.randint(choose_key, array_shape, 0, 1000)
    classes = jnp.where(choose < 700, block_major, classes)
    chance = jax.random.randint(drop_key, array_shape, 0, 1000)
    drop_limit = 40 + 700 * row_index * row_index // (QUARTER_ROWS * QUARTER_ROWS)
    return jnp.where(chance < drop_limit[None, :, None], 255, classes).astype(jnp.int32)


def centred(key, dims, scale, bound, held_as=jnp.bfloat16):
    drawn = jax.random.normal(key, dims, jnp.float32) * scale
    return jnp.minimum(jnp.maximum(drawn, -bound), bound).astype(held_as)


def setup_inputs(seed: int = 0) -> dict:
    arg_keys = jax.random.split(jax.random.key(seed), 12)
    feat_quarter = draw_feat_quarter(jax.random.fold_in(arg_keys[11], 71), 0)
    feat_eighth = draw_feat_eighth(jax.random.fold_in(arg_keys[11], 71), 0)
    feat_sixteenth = draw_feat_sixteenth(jax.random.fold_in(arg_keys[11], 71), 0)
    feat_thirty = draw_feat_thirty(jax.random.fold_in(arg_keys[11], 71), 0)
    labels = draw_labels(jax.random.fold_in(arg_keys[11], 71), 0)
    first_weights = centred(arg_keys[5], (4, 3, 3, C_IN, HEAD), (9 * C_IN) ** -0.5, 0.125)
    inner_weights = centred(arg_keys[6], (3, 3, 3, HEAD, HEAD), (9 * HEAD) ** -0.5, 0.1875)
    norm_gain = jnp.clip(1.0 + 0.18 * jax.random.normal(arg_keys[7], (7, HEAD), jnp.float32), 0.1, 1.9)
    norm_shift = centred(arg_keys[8], (7, HEAD), 0.5, 3.0, jnp.float32)
    class_weight = centred(arg_keys[9], (HEAD, CLASSES), HEAD ** -0.5, 0.5)
    class_bias = centred(arg_keys[10], (CLASSES,), 0.5, 3.0, jnp.float32)
    return {"feat_quarter": feat_quarter, "feat_eighth": feat_eighth, "feat_sixteenth": feat_sixteenth, "feat_thirty": feat_thirty, "labels": labels, "first_weights": first_weights, "inner_weights": inner_weights, "norm_gain": norm_gain, "norm_shift": norm_shift, "class_weight": class_weight, "class_bias": class_bias}


NORM_FLOOR = 0.05

def conv_rows(framed, weight):
    row_count = framed.shape[0] - 2
    col_count = framed.shape[1]
    padded = jnp.pad(framed, ((0, 0), (1, 1), (0, 0)))
    result = jnp.zeros((row_count, col_count, weight.shape[3]), jnp.float32)
    for downward in range(3):
        for across in range(3):
            window = padded[downward:downward + row_count, across:across + col_count, :]
            result = result + jnp.einsum('rwc,cd->rwd', window.astype(jnp.float32), weight[downward, across].astype(jnp.float32))
    return result

def heighten(padded):
    row_count = padded.shape[0] - 2
    middle = padded[1:-1]
    even_rows = 0.75 * middle + 0.25 * padded[:-2]
    odd_rows = 0.75 * middle + 0.25 * padded[2:]
    inner_rows = jnp.stack([even_rows, odd_rows], axis=1).reshape(2 * row_count, padded.shape[1], padded.shape[2])
    upper_row = 0.75 * padded[0] + 0.25 * padded[1]
    lower_row = 0.75 * padded[-1] + 0.25 * padded[-2]
    return jnp.concatenate([upper_row[None], inner_rows, lower_row[None]], axis=0)

def widen(field):
    left_side = jnp.concatenate([field[:, :1], field[:, :-1]], axis=1)
    right_side = jnp.concatenate([field[:, 1:], field[:, -1:]], axis=1)
    even_cols = 0.75 * field + 0.25 * left_side
    odd_cols = 0.75 * field + 0.25 * right_side
    return jnp.stack([even_cols, odd_cols], axis=2).reshape(field.shape[0], 2 * field.shape[1], field.shape[2])

def group_sum(values):
    channel_sums = lax.optimization_barrier(jnp.sum(values, axis=(0, 1)))
    return channel_sums.reshape(GROUPS, -1).sum(axis=1)

def spread(values, width):
    return jnp.repeat(values, width // GROUPS)

def finish(values, group_mean, group_var, gain, shift):
    width = values.shape[2]
    factor = gain * lax.rsqrt(spread(group_var, width) + NORM_FLOOR)
    return jnp.maximum((values - spread(group_mean, width)) * factor + shift, 0.0).astype(jnp.bfloat16)

def normalize(values, gain, shift):
    pixels = values.shape[0] * values.shape[1] * (values.shape[2] // GROUPS)
    group_mean = group_sum(values) / pixels
    centered = values - spread(group_mean, values.shape[2])
    group_var = group_sum(centered * centered) / pixels
    return finish(values, group_mean, group_var, gain, shift)

def upsample(active):
    padded = jnp.pad(active, ((1, 1), (0, 0), (0, 0)), mode='edge').astype(jnp.float32)
    return widen(heighten(padded)[1:-1]).astype(jnp.bfloat16)

def reference(feat_quarter, feat_eighth, feat_sixteenth, feat_thirty, labels, first_weights, inner_weights, norm_gain, norm_shift, class_weight, class_bias):

    def section(image_in, weight, layer_index):
        framed = jnp.pad(image_in, ((1, 1), (0, 0), (0, 0)))
        return normalize(conv_rows(framed, weight), norm_gain[layer_index], norm_shift[layer_index])

    def one_image(image_items):
        quarter_in, eighth_in, sixteenth_in, thirty_in, label_map = image_items
        quarter = section(quarter_in, first_weights[0], 0)
        eighth = upsample(section(eighth_in, first_weights[1], 1))
        sixteenth = upsample(section(upsample(section(sixteenth_in, first_weights[2], 2)), inner_weights[0], 4))
        coarse = upsample(section(thirty_in, first_weights[3], 3))
        thirty = upsample(section(upsample(section(coarse, inner_weights[1], 5)), inner_weights[2], 6))
        combined = (quarter.astype(jnp.float32) + eighth.astype(jnp.float32) + sixteenth.astype(jnp.float32) + thirty.astype(jnp.float32)).astype(jnp.bfloat16)
        scores = jnp.einsum('rwc,ck->krw', combined.astype(jnp.float32), class_weight.astype(jnp.float32)) + class_bias.astype(jnp.float32)[:, None, None]
        log_total = jnp.log(lax.optimization_barrier(jnp.sum(jnp.exp(scores), axis=0)))
        classes = jnp.arange(scores.shape[0], dtype=jnp.int32)[:, None, None]
        picked = lax.optimization_barrier(jnp.sum(jnp.where(classes == label_map[None], scores, 0.0), axis=0))
        usable = label_map != 255
        loss_total = jnp.sum(jnp.where(usable, log_total - picked, 0.0))
        valid_count = jnp.sum(usable.astype(jnp.float32))
        return (scores.astype(jnp.bfloat16), loss_total, valid_count)
    logits, totals, counts = lax.map(one_image, (feat_quarter, feat_eighth, feat_sixteenth, feat_thirty, labels))
    mean_loss = jnp.sum(totals) / jnp.maximum(jnp.sum(counts), 1.0)
    return (logits, mean_loss)
```

```python
import functools

import jax
import jax.numpy as jnp
from jax import lax
from jax.experimental import pallas as pl
from jax.experimental.pallas import tpu as pltpu
from jax.sharding import PartitionSpec as P

MESH = pl.DeviceIdType.MESH
FLOOR = 0.05
CLASSES = 19
F32 = jnp.float32
BF16 = jnp.bfloat16


def group_total(tile):
    lane = lax.broadcasted_iota(jnp.int32, tile.shape, 1)
    tile = tile + jnp.where(lane % 2 == 0, pltpu.roll(tile, 127, 1), pltpu.roll(tile, 1, 1))
    return tile + jnp.where(lane % 4 < 2, pltpu.roll(tile, 126, 1), pltpu.roll(tile, 2, 1))


def double_matrix(width, out_axis):
    shape = (2 * width, width) if out_axis == 0 else (width, 2 * width)
    out = lax.broadcasted_iota(jnp.int32, shape, out_axis)
    src = lax.broadcasted_iota(jnp.int32, shape, 1 - out_axis)
    half = out // 2
    other = jnp.clip(half + 2 * (out % 2) - 1, 0, width - 1)
    return jnp.where(src == half, 0.75, 0.0) + jnp.where(src == other, 0.25, 0.0)


def kernel(
    nb, nr,
    xq_hbm, x8_hbm, x16_hbm, x32_hbm, lab_hbm, fw_hbm, iw_hbm, gain_hbm, shift_hbm, cw_hbm, cb_hbm,
    out_ref, loss_ref,
    xq, x8, x16, x32, lab, fw, iw, gain, shift, cw, cb,
    yq, y8, y16, y32, y4, y5, y6,
    a16, a32, a5, in4, in5, in6,
    p512, p256, p128, p64,
    u64, u128, u256, cwf, wct, bias,
    qt, zt, zc, sums, picks, tall,
    stats, loss_rows, loss_batch,
    local_sem, halo_send, halo_recv, stat_send, stat_recv, loss_send, loss_recv,
):
    pos = lax.axis_index("rows")
    bat = lax.axis_index("batch")
    last = nr - 1

    def local(src, dst, index):
        return pltpu.make_async_copy(src, dst, local_sem.at[index])

    copies = {
        "fw3": local(fw_hbm.at[3], fw.at[3], 0),
        "x32": local(x32_hbm.at[0], x32.at[pl.ds(3, 2)], 1),
        "fw0": local(fw_hbm.at[0], fw.at[0], 2),
        "xqa": local(xq_hbm.at[0, pl.ds(0, 8)], xq.at[pl.ds(1, 8)], 3),
        "xqb": local(xq_hbm.at[0, pl.ds(8, 8)], xq.at[pl.ds(9, 8)], 4),
        "gain": local(gain_hbm, gain, 5),
        "shift": local(shift_hbm, shift, 6),
        "cw": local(cw_hbm, cw, 7),
        "cb": local(cb_hbm, cb, 8),
        "fw2": local(fw_hbm.at[2], fw.at[2], 9),
        "x16": local(x16_hbm.at[0], x16.at[pl.ds(3, 4)], 10),
        "iw": local(iw_hbm, iw, 11),
        "fw1": local(fw_hbm.at[1], fw.at[1], 12),
        "x8": local(x8_hbm.at[0], x8.at[pl.ds(2, 8)], 13),
        "lab": local(lab_hbm.at[0], lab, 14),
    }

    barrier = pltpu.get_barrier_semaphore()

    def greet_row(k, carry):
        pl.semaphore_signal(
            barrier, inc=1, device_id={"rows": lax.rem(pos + k, nr)}, device_id_type=MESH
        )
        return carry

    def greet_batch(k, carry):
        pl.semaphore_signal(
            barrier, inc=1, device_id={"batch": lax.rem(bat + k, nb)}, device_id_type=MESH
        )
        return carry

    lax.fori_loop(1, nr, greet_row, 0)
    lax.fori_loop(1, nb, greet_batch, 0)
    for name in ("fw0", "xqa", "xqb", "x32", "fw3", "cw", "cb", "gain", "shift", "fw2", "x16", "iw",
                 "fw1", "x8", "lab"):
        copies[name].start()

    m64 = double_matrix(64, 0)
    u64[:, 0:64] = 0.75 * m64
    u64[:, 64:128] = 0.25 * m64
    m128 = double_matrix(128, 0)
    u128[:, 0:128] = (0.75 * m128).astype(BF16)
    u128[:, 128:256] = (0.25 * m128).astype(BF16)
    u256[...] = double_matrix(256, 1).astype(BF16)
    for scratch, width in ((p512, 512), (p256, 256), (p128, 128), (p64, 64)):
        rows = scratch.shape[1]
        scratch[:, :, 0:8, :] = jnp.zeros((2, rows, 8, 128), F32)
        scratch[:, :, width + 8 : width + 16, :] = jnp.zeros((2, rows, 8, 128), F32)

    @pl.when(pos == 0)
    def _():
        xq[0] = jnp.zeros_like(xq[0])
        x8[0:2] = jnp.zeros_like(x8[0:2])
        x16[0:3] = jnp.zeros_like(x16[0:3])
        x32[0:3] = jnp.zeros_like(x32[0:3])

    @pl.when(pos == 1)
    def _():
        x32[0] = jnp.zeros_like(x32[0])

    @pl.when(pos == last)
    def _():
        xq[17] = jnp.zeros_like(xq[17])
        x8[10:12] = jnp.zeros_like(x8[10:12])
        x16[7:10] = jnp.zeros_like(x16[7:10])
        x32[5:8] = jnp.zeros_like(x32[5:8])

    @pl.when(pos == last - 1)
    def _():
        x32[7] = jnp.zeros_like(x32[7])

    copies["cw"].wait()
    copies["cb"].wait()
    cwf[...] = jnp.zeros_like(cwf)
    cwf[:, 0:CLASSES] = cw[...].astype(F32)
    wct[...] = jnp.transpose(cwf[...])[0:32].astype(BF16)
    cwf[...] = jnp.zeros_like(cwf)
    cwf[0:1, 0:CLASSES] = cb[...]
    bias[...] = jnp.broadcast_to(jnp.transpose(cwf[...])[0:32, 0:1], (32, 512))

    pl.semaphore_wait(barrier, nr - 1 + nb - 1)

    def halo(src, dst, index, step):
        return pltpu.make_async_remote_copy(
            src_ref=src, dst_ref=dst, send_sem=halo_send.at[index], recv_sem=halo_recv.at[index],
            device_id={"rows": pos + step}, device_id_type=MESH,
        )

    def halos(name):
        if name == "t1":
            return (halo(x32_hbm.at[0], x32.at[pl.ds(1, 2)], 0, 1),
                    halo(x32_hbm.at[0], x32.at[pl.ds(5, 2)], 1, -1), 1)
        if name == "t2":
            return (halo(x32_hbm.at[0, pl.ds(1, 1)], x32.at[pl.ds(0, 1)], 2, 2),
                    halo(x32_hbm.at[0, pl.ds(0, 1)], x32.at[pl.ds(7, 1)], 3, -2), 2)
        if name == "s":
            return (halo(x16_hbm.at[0, pl.ds(1, 3)], x16.at[pl.ds(0, 3)], 4, 1),
                    halo(x16_hbm.at[0, pl.ds(0, 3)], x16.at[pl.ds(7, 3)], 5, -1), 1)
        if name == "e":
            return (halo(x8_hbm.at[0, pl.ds(6, 2)], x8.at[pl.ds(0, 2)], 6, 1),
                    halo(x8_hbm.at[0, pl.ds(0, 2)], x8.at[pl.ds(10, 2)], 7, -1), 1)
        return (halo(xq_hbm.at[0, pl.ds(15, 1)], xq.at[pl.ds(0, 1)], 8, 1),
                halo(xq_hbm.at[0, pl.ds(0, 1)], xq.at[pl.ds(17, 1)], 9, -1), 1)

    def halo_start(name):
        down, up, step = halos(name)
        pl.when(pos + step <= last)(down.start)
        pl.when(pos - step >= 0)(up.start)

    def halo_wait(name):
        down, up, step = halos(name)
        pl.when(pos - step >= 0)(down.wait_recv)
        pl.when(pos + step <= last)(up.wait_recv)

    def halo_sent(name):
        down, up, step = halos(name)
        pl.when(pos + step <= last)(down.wait_send)
        pl.when(pos - step >= 0)(up.wait_send)

    for name in ("t1", "t2", "s", "e", "q"):
        halo_start(name)

    def conv(x_ref, in_off, w_ref, y_ref, first, count, width, per_step, pad):
        depth = x_ref.shape[2]

        def step(i, carry):
            row = first + i * per_step
            lhs = jnp.concatenate(
                [x_ref[pl.ds(in_off + row + dr, per_step)].reshape(per_step * width, depth)
                 for dr in range(3)], axis=1)
            rhs = jnp.concatenate(
                [jnp.concatenate([w_ref[dr, dc] for dc in range(3)], axis=1) for dr in range(3)],
                axis=0)
            part = jnp.dot(lhs, rhs, preferred_element_type=F32)
            shape = (per_step, width, 128)
            pad[0, :, 8 : 8 + width, :] = part[:, 0:128].reshape(shape)
            pad[1, :, 8 : 8 + width, :] = part[:, 256:384].reshape(shape)
            y_ref[pl.ds(row, per_step)] = (
                part[:, 128:256].reshape(shape)
                + pad[0, :, 7 : 7 + width, :]
                + pad[1, :, 9 : 9 + width, :]
            )
            return carry

        lax.fori_loop(0, count // per_step, step, 0)

    def moments(y_ref, first, count, width, layer):
        def add(i, acc):
            return acc + jnp.sum(y_ref[first + i].reshape(width // 8, 8, 128), axis=0)

        total = lax.fori_loop(0, count, add, jnp.zeros((8, 128), F32))
        total = jnp.broadcast_to(jnp.sum(total, axis=0, keepdims=True), (8, 128))
        mean = group_total(total) * (1.0 / (count * width * 4))

        def add_square(i, acc):
            off = y_ref[first + i].reshape(width // 8, 8, 128) - mean[None]
            return acc + jnp.sum(off * off, axis=0)

        square = lax.fori_loop(0, count, add_square, jnp.zeros((8, 128), F32))
        square = jnp.broadcast_to(jnp.sum(square, axis=0, keepdims=True), (8, 128))
        square = group_total(square)
        sub = lax.broadcasted_iota(jnp.int32, (8, 128), 0)
        stats[layer, pos] = jnp.where(sub == 0, mean, square)

        def send(k, carry):
            stat_copy(layer, lax.rem(pos + k, nr)).start()
            return carry

        lax.fori_loop(1, nr, send, 0)

    def stat_copy(layer, peer):
        return pltpu.make_async_remote_copy(
            src_ref=stats.at[layer, pos], dst_ref=stats.at[layer, pos],
            send_sem=stat_send.at[layer], recv_sem=stat_recv.at[layer],
            device_id={"rows": peer}, device_id_type=MESH,
        )

    def tiles_wait(ref, sem):
        pltpu.make_async_copy(ref, ref, sem).wait()

    def scales(layer, local_count):
        tiles_wait(stats.at[layer, pl.ds(0, nr - 1)], stat_recv.at[layer])
        every = [stats[layer, i] for i in range(nr)]
        total = functools.reduce(lambda a, b: a + b, every)
        mean = total[0:1] * (1.0 / nr)
        spread = [(tile[0:1] - mean) * (tile[0:1] - mean) for tile in every]
        square = total[1:2] + local_count * functools.reduce(lambda a, b: a + b, spread)
        var = square * (1.0 / (nr * local_count))
        factor = gain[pl.ds(layer, 1), :] * lax.rsqrt(var + FLOOR)
        return mean, factor, shift[pl.ds(layer, 1), :]

    def activate(values, scale):
        mean, factor, offset = scale
        return jnp.maximum((values - mean) * factor + offset, 0.0).astype(BF16)

    def normalize(y_ref, a_ref, scale, rows, top, bottom):
        for r in range(rows):
            a_ref[r] = activate(y_ref[r], scale)

        @pl.when(pos == 0)
        def _():
            a_ref[top] = a_ref[top + 1]

        @pl.when(pos == last)
        def _():
            a_ref[bottom] = a_ref[bottom - 1]

    def double(a_ref, u_ref, in_ref, pairs, base, width):
        top_row = a_ref.shape[0] - 1
        for j in range(pairs):
            k = base + j
            mid = a_ref[k]
            rhs = jnp.concatenate(
                [jnp.concatenate([mid, mid], axis=1),
                 jnp.concatenate([a_ref[max(k - 1, 0)], a_ref[min(k + 1, top_row)]], axis=1)],
                axis=0)
            both = jnp.dot(u_ref[...].astype(BF16), rhs, preferred_element_type=F32).astype(BF16)
            in_ref[2 * j] = both[:, 0:128]
            in_ref[2 * j + 1] = both[:, 128:256]

    def clear_outside(in_ref, top_rows, bottom_row):
        @pl.when(pos == 0)
        def _():
            in_ref[0:top_rows] = jnp.zeros_like(in_ref[0:top_rows])

        @pl.when(pos == last)
        def _():
            rest = in_ref.shape[0] - bottom_row
            in_ref[bottom_row:] = jnp.zeros((rest,) + in_ref.shape[1:], BF16)

    nt = (((1,), (1,)), ((), ()))

    copies["fw0"].wait()
    copies["xqa"].wait()
    conv(xq, 0, fw.at[0], yq, 1, 6, 512, 2, p512)

    copies["fw3"].wait()
    copies["x32"].wait()
    halo_wait("t1")
    halo_wait("t2")
    conv(x32, 0, fw.at[3], y32, 0, 6, 64, 6, p64)
    moments(y32, 2, 2, 64, 3)

    copies["fw2"].wait()
    copies["x16"].wait()
    halo_wait("s")
    conv(x16, 0, fw.at[2], y16, 0, 8, 128, 4, p128)
    moments(y16, 2, 4, 128, 2)

    copies["xqb"].wait()
    conv(xq, 0, fw.at[0], yq, 7, 4, 512, 2, p512)

    copies["gain"].wait()
    copies["shift"].wait()
    copies["iw"].wait()
    normalize(y32, a32, scales(3, 2 * 64 * 4), 6, 1, 4)
    double(a32, u64, in5, 6, 0, 64)
    clear_outside(in5, 4, 8)
    conv(in5, 1, iw.at[1], y5, 0, 8, 128, 4, p128)
    moments(y5, 2, 4, 128, 5)

    normalize(y16, a16, scales(2, 4 * 128 * 4), 8, 1, 6)
    double(a16, u128, in4, 6, 1, 128)
    clear_outside(in4, 2, 10)
    conv(in4, 0, iw.at[0], y4, 0, 10, 256, 2, p256)
    moments(y4, 1, 8, 256, 4)

    copies["fw1"].wait()
    copies["x8"].wait()
    halo_wait("e")
    conv(x8, 0, fw.at[1], y8, 0, 10, 256, 2, p256)
    moments(y8, 1, 8, 256, 1)

    normalize(y5, a5, scales(5, 4 * 128 * 4), 8, 1, 6)
    double(a5, u128, in6, 6, 1, 128)
    clear_outside(in6, 2, 10)
    conv(in6, 0, iw.at[2], y6, 0, 10, 256, 2, p256)
    moments(y6, 1, 8, 256, 6)

    conv(xq, 0, fw.at[0], yq, 11, 4, 512, 2, p512)
    halo_wait("q")

    def edge(i, carry):
        row = i * 15
        lhs = jnp.concatenate([xq[row + dr] for dr in range(3)], axis=1)
        rhs = jnp.concatenate(
            [jnp.concatenate([fw[0, dr, dc] for dc in range(3)], axis=1) for dr in range(3)], axis=0)
        part = jnp.dot(lhs, rhs, preferred_element_type=F32)
        p512[0, 0, 8:520, :] = part[:, 0:128]
        p512[1, 0, 8:520, :] = part[:, 256:384]
        yq[row] = part[:, 128:256] + p512[0, 0, 7:519, :] + p512[1, 0, 9:521, :]
        return carry

    lax.fori_loop(0, 2, edge, 0)
    moments(yq, 0, 16, 512, 0)

    def project(y_ref, scale, fresh):
        def step(r, carry):
            act = activate(y_ref[r], scale)
            part = lax.dot_general(wct[...], act, nt, preferred_element_type=F32)
            zt[r] = part if fresh else zt[r] + part
            return carry

        lax.fori_loop(0, 10, step, 0)

    project(y4, scales(4, 8 * 256 * 4), True)
    project(y8, scales(1, 8 * 256 * 4), False)
    project(y6, scales(6, 8 * 256 * 4), False)

    @pl.when(pos == 0)
    def _():
        zt[0] = zt[1]

    @pl.when(pos == last)
    def _():
        zt[9] = zt[8]

    flat = zt[...].reshape(320, 256)
    high = flat.astype(BF16)
    low = (flat - high.astype(F32)).astype(BF16)
    zc[...] = (
        jnp.dot(high, u256[...], preferred_element_type=F32)
        + jnp.dot(low, u256[...], preferred_element_type=F32)
    ).reshape(10, 32, 512)

    scale_q = scales(0, 16 * 512 * 4)
    copies["lab"].wait()

    def finish(r, carry):
        act = activate(yq[r], scale_q)
        main = lax.dot_general(wct[...], act, nt, preferred_element_type=F32)
        half = r // 2
        near = half + 2 * (r % 2)
        score = main + 0.75 * zc[half + 1] + 0.25 * zc[near] + bias[...]
        kind = lax.broadcasted_iota(jnp.int32, (32, 512), 0)
        grown = jnp.where(kind < CLASSES, jnp.exp(score), 0.0)
        sums[pl.ds(r, 1), :] = jnp.sum(grown, axis=0, keepdims=True)
        marks = jnp.broadcast_to(lab[pl.ds(r, 1), :], (32, 512))
        picks[pl.ds(r, 1), :] = jnp.sum(jnp.where(kind == marks, score, 0.0), axis=0, keepdims=True)
        for block in range(4):
            tall[block, pl.ds(r * 36, 32), :] = score[:, block * 128 : (block + 1) * 128]
        return carry

    lax.fori_loop(0, 16, finish, 0)
    usable = lab[...] != 255
    terms = jnp.where(usable, jnp.log(sums[...]) - picks[...], 0.0)
    local_total = jnp.sum(terms)
    local_count = jnp.sum(usable.astype(F32))
    sub = lax.broadcasted_iota(jnp.int32, (8, 128), 0)
    loss_rows[pos] = jnp.where(sub == 0, local_total, local_count)

    def loss_copy(ref, slot, index, target):
        return pltpu.make_async_remote_copy(
            src_ref=ref.at[slot], dst_ref=ref.at[slot],
            send_sem=loss_send.at[index], recv_sem=loss_recv.at[index],
            device_id=target, device_id_type=MESH,
        )

    def send_row(k, carry):
        loss_copy(loss_rows, pos, 0, {"rows": lax.rem(pos + k, nr)}).start()
        return carry

    lax.fori_loop(1, nr, send_row, 0)

    for k in range(CLASSES):
        for block in range(4):
            out_ref[0, k, :, block * 128 : (block + 1) * 128] = tall[
                block, pl.ds(k, 16, stride=36), :
            ].astype(BF16)

    tiles_wait(loss_rows.at[pl.ds(0, nr - 1)], loss_recv.at[0])
    loss_batch[bat] = functools.reduce(lambda a, b: a + b, [loss_rows[i] for i in range(nr)])

    def send_batch(k, carry):
        loss_copy(loss_batch, bat, 1, {"batch": lax.rem(bat + k, nb)}).start()
        return carry

    lax.fori_loop(1, nb, send_batch, 0)

    for name in ("t1", "t2", "s", "e", "q"):
        halo_sent(name)
    for layer in range(7):
        tiles_wait(stats.at[layer, pl.ds(0, nr - 1)], stat_send.at[layer])
    tiles_wait(loss_rows.at[pl.ds(0, nr - 1)], loss_send.at[0])
    tiles_wait(loss_batch.at[pl.ds(0, nb - 1)], loss_recv.at[1])
    whole = functools.reduce(lambda a, b: a + b, [loss_batch[i] for i in range(nb)])
    loss_ref[...] = whole[0:1] / jnp.maximum(whole[1:2], 1.0)
    tiles_wait(loss_batch.at[pl.ds(0, nb - 1)], loss_send.at[1])


def solution(mesh):
    nb, nr = mesh.shape["batch"], mesh.shape["rows"]

    def per_device(xq, x8, x16, x32, labels, fw, iw, gain, shift, cw, cb):
        any_spec = pl.BlockSpec(memory_space=pl.ANY)
        vmem = pl.BlockSpec(memory_space=pltpu.VMEM)
        V = pltpu.VMEM
        logits, loss = pl.pallas_call(
            functools.partial(kernel, nb, nr),
            out_shape=(
                jax.ShapeDtypeStruct((1, CLASSES, 16, 512), BF16),
                jax.ShapeDtypeStruct((1, 128), F32),
            ),
            in_specs=[any_spec] * 11,
            out_specs=(vmem, vmem),
            scratch_shapes=[
                V((18, 512, 256), BF16), V((12, 256, 256), BF16), V((10, 128, 256), BF16),
                V((8, 64, 256), BF16), V((16, 512), jnp.int32), V((4, 3, 3, 256, 128), BF16),
                V((3, 3, 3, 128, 128), BF16), V((7, 128), F32), V((7, 128), F32),
                V((128, CLASSES), BF16), V((1, CLASSES), F32),
                V((16, 512, 128), F32), V((10, 256, 128), F32), V((8, 128, 128), F32),
                V((6, 64, 128), F32), V((10, 256, 128), F32), V((8, 128, 128), F32),
                V((10, 256, 128), F32),
                V((8, 128, 128), BF16), V((6, 64, 128), BF16), V((8, 128, 128), BF16),
                V((12, 256, 128), BF16), V((12, 128, 128), BF16), V((12, 256, 128), BF16),
                V((2, 2, 528, 128), F32), V((2, 2, 272, 128), F32), V((2, 4, 144, 128), F32),
                V((2, 6, 80, 128), F32),
                V((128, 128), F32), V((256, 256), BF16), V((256, 512), BF16),
                V((128, 128), F32), V((32, 128), BF16), V((32, 512), F32),
                V((16, 32, 512), F32), V((10, 32, 256), F32), V((10, 32, 512), F32),
                V((16, 512), F32), V((16, 512), F32), V((4, 16 * 36, 128), F32),
                V((7, nr, 8, 128), F32), V((nr, 8, 128), F32), V((nb, 8, 128), F32),
                pltpu.SemaphoreType.DMA((15,)), pltpu.SemaphoreType.DMA((10,)),
                pltpu.SemaphoreType.DMA((10,)), pltpu.SemaphoreType.DMA((7,)),
                pltpu.SemaphoreType.DMA((7,)), pltpu.SemaphoreType.DMA((2,)),
                pltpu.SemaphoreType.DMA((2,)),
            ],
            compiler_params=pltpu.CompilerParams(
                collective_id=0, has_side_effects=True, vmem_limit_bytes=60 * 1024 * 1024
            ),
        )(xq, x8, x16, x32, labels, fw, iw, gain, shift, cw, cb.reshape(1, CLASSES))
        return logits, loss[0, 0]

    batch, rows = "batch", "rows"
    return jax.shard_map(
        per_device, mesh=mesh,
        in_specs=(P(batch, rows, None, None),) * 4 + (P(batch, rows, None),) + (P(),) * 6,
        out_specs=(P(batch, None, rows, None), P()),
        check_vma=False,
    )
```

```python
import functools

import jax
import jax.numpy as jnp
from jax import lax
from jax.experimental import pallas as pl
from jax.experimental.pallas import tpu as pltpu
from jax.sharding import PartitionSpec as P

MESH = pl.DeviceIdType.MESH
FLOOR = 0.05
CLASSES = 19
F32 = jnp.float32
BF16 = jnp.bfloat16


def group_total(tile):
    lane = lax.broadcasted_iota(jnp.int32, tile.shape, 1)
    tile = tile + jnp.where(lane % 2 == 0, pltpu.roll(tile, 127, 1), pltpu.roll(tile, 1, 1))
    return tile + jnp.where(lane % 4 < 2, pltpu.roll(tile, 126, 1), pltpu.roll(tile, 2, 1))


def double_matrix(width, out_axis):
    shape = (2 * width, width) if out_axis == 0 else (width, 2 * width)
    out = lax.broadcasted_iota(jnp.int32, shape, out_axis)
    src = lax.broadcasted_iota(jnp.int32, shape, 1 - out_axis)
    half = out // 2
    other = jnp.clip(half + 2 * (out % 2) - 1, 0, width - 1)
    return jnp.where(src == half, 0.75, 0.0) + jnp.where(src == other, 0.25, 0.0)


def kernel(
    nb, nr,
    xq_hbm, x8_hbm, x16_hbm, x32_hbm, lab_hbm, fw_hbm, iw_hbm, gain_hbm, shift_hbm, cw_hbm, cb_hbm,
    out_hbm, loss_ref,
    xq, x8, x16, x32, lab, fw, iw, gain, shift, cw, cb,
    yq, y8, y16, y32, y4, y5, y6,
    a16, a32, a5, in4, in5, in6,
    p512, p256, p128, p64,
    u64, u128, u256, cwf, wct, bias,
    zt, ze, zc, sums, picks, tall, out,
    moms, stats, loss_rows, loss_batch,
    local_sem, halo_send, halo_recv, stat_send, stat_recv, loss_send, loss_recv,
):
    pos = lax.axis_index("rows")
    bat = lax.axis_index("batch")
    last = nr - 1
    scope = jax.named_scope

    def local(src, dst, index):
        return pltpu.make_async_copy(src, dst, local_sem.at[index])

    copies = {
        "fw0": local(fw_hbm.at[0], fw.at[0], 2),
        "xqa": local(xq_hbm.at[0, pl.ds(0, 6)], xq.at[pl.ds(1, 6)], 3),
        "x32": local(x32_hbm.at[0], x32.at[pl.ds(3, 2)], 1),
        "x16": local(x16_hbm.at[0], x16.at[pl.ds(2, 4)], 10),
        "fw3": local(fw_hbm.at[3], fw.at[3], 0),
        "xqb": local(xq_hbm.at[0, pl.ds(6, 10)], xq.at[pl.ds(7, 10)], 4),
        "fw2": local(fw_hbm.at[2], fw.at[2], 9),
        "gain": local(gain_hbm, gain, 5),
        "shift": local(shift_hbm, shift, 6),
        "iw": local(iw_hbm, iw, 11),
        "x8": local(x8_hbm.at[0], x8.at[pl.ds(1, 8)], 13),
        "fw1": local(fw_hbm.at[1], fw.at[1], 12),
        "cw": local(cw_hbm, cw, 7),
        "cb": local(cb_hbm, cb, 8),
        "lab": local(lab_hbm.at[0], lab, 14),
    }

    barrier = pltpu.get_barrier_semaphore()

    def greet_row(k, carry):
        pl.semaphore_signal(
            barrier, inc=1, device_id={"rows": lax.rem(pos + k, nr)}, device_id_type=MESH
        )
        return carry

    def greet_batch(k, carry):
        pl.semaphore_signal(
            barrier, inc=1, device_id={"batch": lax.rem(bat + k, nb)}, device_id_type=MESH
        )
        return carry

    with scope("greet"):
        lax.fori_loop(1, nr, greet_row, 0)
        lax.fori_loop(1, nb, greet_batch, 0)
    with scope("local_start"):
        for copy in copies.values():
            copy.start()

    with scope("constants"):
        m64 = double_matrix(64, 0)
        u64[:, 0:64] = 0.75 * m64
        u64[:, 64:128] = 0.25 * m64
        m128 = double_matrix(128, 0)
        u128[:, 0:128] = (0.75 * m128).astype(BF16)
        u128[:, 128:256] = (0.25 * m128).astype(BF16)
        for scratch, width in ((p512, 512), (p256, 256), (p128, 128), (p64, 64)):
            rows = scratch.shape[2]
            scratch[:, :, :, 0:8, :] = jnp.zeros((2, 2, rows, 8, 128), F32)
            scratch[:, :, :, width + 8 : width + 16, :] = jnp.zeros((2, 2, rows, 8, 128), F32)

        @pl.when(pos == 0)
        def _():
            xq[0] = jnp.zeros_like(xq[0])
            x8[0] = jnp.zeros_like(x8[0])
            x16[0:2] = jnp.zeros_like(x16[0:2])
            x32[0:3] = jnp.zeros_like(x32[0:3])

        @pl.when(pos == 1)
        def _():
            x32[0] = jnp.zeros_like(x32[0])

        @pl.when(pos == last)
        def _():
            xq[17] = jnp.zeros_like(xq[17])
            x8[9] = jnp.zeros_like(x8[9])
            x16[6:8] = jnp.zeros_like(x16[6:8])
            x32[5:8] = jnp.zeros_like(x32[5:8])

        @pl.when(pos == last - 1)
        def _():
            x32[7] = jnp.zeros_like(x32[7])

    with scope("barrier"):
        copies["x32"].wait()
        copies["x16"].wait()
        pl.semaphore_wait(barrier, nr - 1 + nb - 1)

    def remote(src, dst, index, step):
        return pltpu.make_async_remote_copy(
            src_ref=src, dst_ref=dst, send_sem=halo_send.at[index], recv_sem=halo_recv.at[index],
            device_id={"rows": pos + step}, device_id_type=MESH,
        )

    def halos(name, piece=None):
        if name == "t1":
            return (remote(x32.at[pl.ds(3, 2)], x32.at[pl.ds(1, 2)], 0, 1),
                    remote(x32.at[pl.ds(3, 2)], x32.at[pl.ds(5, 2)], 1, -1), 1)
        if name == "t2":
            return (remote(x32.at[pl.ds(4, 1)], x32.at[pl.ds(0, 1)], 2, 2),
                    remote(x32.at[pl.ds(3, 1)], x32.at[pl.ds(7, 1)], 3, -2), 2)
        if name == "s":
            return (remote(x16.at[pl.ds(4, 2)], x16.at[pl.ds(0, 2)], 4, 1),
                    remote(x16.at[pl.ds(2, 2)], x16.at[pl.ds(6, 2)], 5, -1), 1)
        if name == "e":
            return (remote(x8.at[pl.ds(8, 1)], x8.at[pl.ds(0, 1)], 6, 1),
                    remote(x8.at[pl.ds(1, 1)], x8.at[pl.ds(9, 1)], 7, -1), 1)
        if name == "z":
            return (remote(zt.at[7], ze.at[0], 10, 1), remote(zt.at[0], ze.at[1], 11, -1), 1)
        cols = pl.ds(0, 512) if piece is None else pl.ds(piece * 128, 128)
        return (remote(xq.at[16, cols], xq.at[0, cols], 8, 1),
                remote(xq.at[1, cols], xq.at[17, cols], 9, -1), 1)

    def halo_start(name, piece=None):
        down, up, step = halos(name, piece)
        pl.when(pos + step <= last)(down.start)
        pl.when(pos - step >= 0)(up.start)

    def halo_wait(name):
        down, up, step = halos(name)
        pl.when(pos - step >= 0)(down.wait_recv)
        pl.when(pos + step <= last)(up.wait_recv)

    def halo_sent(name):
        down, up, step = halos(name)
        pl.when(pos + step <= last)(down.wait_send)
        pl.when(pos - step >= 0)(up.wait_send)

    with scope("send_ts"):
        halo_start("t1")
        halo_start("t2")
        halo_start("s")

    def column_sum(values):
        pixels = values.shape[0]
        values = values.reshape(pixels // 64, 8, 8, 128)
        return jnp.sum(jnp.sum(values, axis=0), axis=0)

    def conv(layer, x_ref, in_off, w_ref, y_ref, steps, width, pads):
        depth = x_ref.shape[2]

        def multiply(index):
            rows = steps[index][0]
            pad = pads.at[index % 2]
            lhs = jnp.concatenate(
                [jnp.concatenate([x_ref[in_off + row + dr] for row in rows], axis=0)
                 for dr in range(3)], axis=1)
            rhs = jnp.concatenate(
                [jnp.concatenate([w_ref[dr, dc] for dc in range(3)], axis=1) for dr in range(3)],
                axis=0)
            part = jnp.dot(lhs, rhs, preferred_element_type=F32)
            for i, row in enumerate(rows):
                here = slice(i * width, (i + 1) * width)
                pad[0, i, 8 : 8 + width, :] = part[here, 0:128]
                pad[1, i, 8 : 8 + width, :] = part[here, 256:384]
                y_ref[row] = part[here, 128:256]

        def settle(index):
            rows, own, slot = steps[index]
            pad = pads.at[index % 2]
            for i, row in enumerate(rows):
                y_ref[row] = y_ref[row] + pad[0, i, 7 : 7 + width, :] + pad[1, i, 9 : 9 + width, :]
            count = len(own) * width
            total = sum(column_sum(y_ref[row]) for row in own)
            mean = jnp.sum(total, axis=0, keepdims=True) * (1.0 / count)
            square = jnp.zeros((8, 128), F32)
            for row in own:
                off = y_ref[row] - mean
                square = square + column_sum(off * off)
            moms[layer, slot, 0:1, :] = mean
            moms[layer, slot, 1:2, :] = jnp.sum(square, axis=0, keepdims=True)

        multiply(0)
        for index in range(1, len(steps)):
            multiply(index)
            settle(index - 1)
        settle(len(steps) - 1)

    def moments(layer, slots, pixels):
        tiles = [moms[layer, i] for i in range(slots)]
        total = functools.reduce(lambda a, b: a + b, tiles)
        channel = total[0:1] * (1.0 / slots)
        share = pixels // slots
        square = total[1:2]
        for tile in tiles:
            square = square + share * (tile[0:1] - channel) * (tile[0:1] - channel)
        channel = jnp.broadcast_to(channel, (8, 128))
        square = jnp.broadcast_to(square, (8, 128))
        mean = group_total(channel) * 0.25
        square = group_total(square + pixels * (channel - mean) * (channel - mean))
        sub = lax.broadcasted_iota(jnp.int32, (8, 128), 0)
        stats[layer, pos] = jnp.where(sub == 0, mean, square)

        def send(k, carry):
            stat_copy(layer, lax.rem(pos + k, nr)).start()
            return carry

        lax.fori_loop(1, nr, send, 0)

    def stat_copy(layer, peer):
        return pltpu.make_async_remote_copy(
            src_ref=stats.at[layer, pos], dst_ref=stats.at[layer, pos],
            send_sem=stat_send.at[layer], recv_sem=stat_recv.at[layer],
            device_id={"rows": peer}, device_id_type=MESH,
        )

    def tiles_wait(ref, sem):
        pltpu.make_async_copy(ref, ref, sem).wait()

    def scales(layer, pixels):
        local_count = 4 * pixels
        with scope(f"stat_wait{layer}"):
            tiles_wait(stats.at[layer, pl.ds(0, nr - 1)], stat_recv.at[layer])
        every = [stats[layer, i] for i in range(nr)]
        total = functools.reduce(lambda a, b: a + b, every)
        mean = total[0:1] * (1.0 / nr)
        spread = [(tile[0:1] - mean) * (tile[0:1] - mean) for tile in every]
        square = total[1:2] + local_count * functools.reduce(lambda a, b: a + b, spread)
        var = square * (1.0 / (nr * local_count))
        factor = gain[pl.ds(layer, 1), :] * lax.rsqrt(var + FLOOR)
        return mean, factor, shift[pl.ds(layer, 1), :]

    def activate(values, scale):
        mean, factor, offset = scale
        return jnp.maximum((values - mean) * factor + offset, 0.0).astype(BF16)

    def normalize(y_ref, a_ref, scale, rows, top, bottom):
        for r in range(rows):
            a_ref[r] = activate(y_ref[r], scale)

        @pl.when(pos == 0)
        def _():
            a_ref[top] = a_ref[top + 1]

        @pl.when(pos == last)
        def _():
            a_ref[bottom] = a_ref[bottom - 1]

    def double(a_ref, u_ref, in_ref, pairs):
        top_row = a_ref.shape[0] - 1
        end = in_ref.shape[0]
        for k, j in pairs:
            mid = a_ref[k]
            rhs = jnp.concatenate(
                [jnp.concatenate([mid, mid], axis=1),
                 jnp.concatenate([a_ref[max(k - 1, 0)], a_ref[min(k + 1, top_row)]], axis=1)],
                axis=0)
            both = jnp.dot(u_ref[...].astype(BF16), rhs, preferred_element_type=F32).astype(BF16)
            if j >= 0:
                in_ref[j] = both[:, 0:128]
            if j + 1 < end:
                in_ref[j + 1] = both[:, 128:256]

    def clear_outside(in_ref, top_rows, bottom_row):
        @pl.when(pos == 0)
        def _():
            in_ref[0:top_rows] = jnp.zeros_like(in_ref[0:top_rows])

        @pl.when(pos == last)
        def _():
            rest = in_ref.shape[0] - bottom_row
            in_ref[bottom_row:] = jnp.zeros((rest,) + in_ref.shape[1:], BF16)

    nt = (((1,), (1,)), ((), ()))

    def quarter(steps):
        conv(0, xq, 0, fw.at[0], yq, [(rows, rows, slot) for rows, slot in steps], 512, p512)

    with scope("q_wait_a"):
        copies["fw0"].wait()
        copies["xqa"].wait()
    with scope("q_a"):
        quarter([((1, 2), 0), ((3, 4), 1)])
    with scope("q_wait_b"):
        copies["xqb"].wait()
    with scope("q_b"):
        quarter([((5, 6), 2), ((7, 8), 3)])

    with scope("t_wait"):
        copies["fw3"].wait()
        halo_wait("t1")
        halo_wait("t2")
    with scope("l3"):
        conv(3, x32, 0, fw.at[3], y32, [(tuple(range(6)), (2, 3), 0)], 64, p64)
        moments(3, 1, 2 * 64)
    copies["x8"].wait()
    halo_start("e")

    with scope("q_c"):
        quarter([((9, 10), 4), ((11, 12), 5)])

    with scope("s_wait"):
        copies["fw2"].wait()
        halo_wait("s")
    with scope("l2"):
        conv(2, x16, 0, fw.at[2], y16, [(tuple(range(6)), (1, 2, 3, 4), 0)], 128, p128)
        moments(2, 1, 4 * 128)
    halo_start("q", 0)

    copies["gain"].wait()
    copies["shift"].wait()
    copies["iw"].wait()
    scale3 = scales(3, 2 * 64)
    with scope("l5"):
        normalize(y32, a32, scale3, 6, 1, 4)
        double(a32, u64, in5, [(1, 0), (2, 2), (3, 4), (4, 6)])
        clear_outside(in5, 2, 6)
        conv(5, in5, 0, iw.at[1], y5, [(tuple(range(6)), (1, 2, 3, 4), 0)], 128, p128)
        moments(5, 1, 4 * 128)
    halo_start("q", 1)

    with scope("q_d"):
        quarter([((13, 14), 6)])
    halo_start("q", 2)

    eight = [((0, 1, 2, 3),) * 2 + (0,), ((4, 5, 6, 7),) * 2 + (1,)]
    with scope("e_wait"):
        copies["fw1"].wait()
        halo_wait("e")
    with scope("l1"):
        conv(1, x8, 0, fw.at[1], y8, eight, 256, p256)
        moments(1, 2, 8 * 256)
    halo_start("q", 3)

    scale2 = scales(2, 4 * 128)
    five = [(0, -1), (1, 1), (2, 3), (3, 5), (4, 7), (5, 9)]
    with scope("l4"):
        normalize(y16, a16, scale2, 6, 0, 5)
        double(a16, u128, in4, five)
        clear_outside(in4, 1, 9)
        conv(4, in4, 0, iw.at[0], y4, eight, 256, p256)
        moments(4, 2, 8 * 256)

    scale5 = scales(5, 4 * 128)
    with scope("l6"):
        normalize(y5, a5, scale5, 6, 0, 5)
        double(a5, u128, in6, five)
        clear_outside(in6, 1, 9)
        conv(6, in6, 0, iw.at[2], y6, eight, 256, p256)
        moments(6, 2, 8 * 256)

    with scope("q_wait_e"):
        halo_wait("q")
    with scope("q_e"):
        quarter([((0, 15), 7)])
        moments(0, 8, 16 * 512)

    with scope("class_consts"):
        copies["cw"].wait()
        copies["cb"].wait()
        copies["lab"].wait()
        u256[...] = double_matrix(256, 1).astype(BF16)
        cwf[...] = jnp.zeros_like(cwf)
        cwf[0:CLASSES, :] = cw[...].astype(F32)
        wct[:, 0:128] = cwf[0:32, :].astype(BF16)
        wct[:, 128:256] = cwf[0:32, :].astype(BF16)
        cwf[...] = jnp.zeros_like(cwf)
        cwf[0:1, 0:CLASSES] = cb[...]
        bias[...] = jnp.broadcast_to(jnp.transpose(cwf[...])[0:32, 0:1], (32, 128))

    scale1 = scales(1, 8 * 256)
    scale4 = scales(4, 8 * 256)
    with scope("z14"):
        for half in range(2):
            act = jnp.concatenate(
                [jnp.concatenate([activate(y4[r], scale4), activate(y8[r], scale1)], axis=1)
                 for r in range(half * 4, half * 4 + 4)], axis=0)
            part = lax.dot_general(wct[...], act, nt, preferred_element_type=F32)
            for i in range(4):
                zt[half * 4 + i] = part[:, i * 256 : (i + 1) * 256]
    scale6 = scales(6, 8 * 256)
    with scope("z6"):
        for half in range(2):
            act = jnp.concatenate(
                [activate(y6[r], scale6) for r in range(half * 4, half * 4 + 4)], axis=0)
            part = lax.dot_general(wct[:, 0:128], act, nt, preferred_element_type=F32)
            for i in range(4):
                zt[half * 4 + i] = zt[half * 4 + i] + part[:, i * 256 : (i + 1) * 256]

    halo_start("z")

    def widen(flat):
        high = flat.astype(BF16)
        low = (flat - high.astype(F32)).astype(BF16)
        return (jnp.dot(high, u256[...], preferred_element_type=F32)
                + jnp.dot(low, u256[...], preferred_element_type=F32))

    with scope("widen"):
        zc[1:9] = widen(zt[...].reshape(256, 256)).reshape(8, 32, 512)

        @pl.when(pos == 0)
        def _():
            ze[0] = zt[0]

        @pl.when(pos == last)
        def _():
            ze[1] = zt[7]

    scale0 = scales(0, 16 * 512)

    def finish(rows):
        act = jnp.concatenate([activate(yq[r], scale0) for r in rows], axis=0)
        main = lax.dot_general(wct[:, 0:128], act, nt, preferred_element_type=F32)
        kind = lax.broadcasted_iota(jnp.int32, (32, 512), 0)
        offset = jnp.concatenate([bias[...]] * 4, axis=1)
        for i, r in enumerate(rows):
            half = r // 2
            near = half + 2 * (r % 2)
            score = (main[:, i * 512 : (i + 1) * 512] + offset
                     + 0.75 * zc[half + 1] + 0.25 * zc[near])
            grown = jnp.where(kind < CLASSES, jnp.exp(score), 0.0)
            sums[r : r + 1, :] = jnp.sum(grown, axis=0, keepdims=True)
            marks = jnp.broadcast_to(lab[r : r + 1, :], (32, 512))
            picks[r : r + 1, :] = jnp.sum(
                jnp.where(kind == marks, score, 0.0), axis=0, keepdims=True)
            for block in range(4):
                tall[block, r * 36 : r * 36 + 32, :] = score[:, block * 128 : (block + 1) * 128]

    with scope("finish"):
        for r in range(1, 15, 2):
            finish((r, r + 1))
    with scope("z_wait"):
        halo_wait("z")
    with scope("finish_edge"):
        edges = widen(jnp.concatenate([ze[0], ze[1]], axis=0))
        zc[0] = edges[0:32]
        zc[9] = edges[32:64]
        finish((0, 15))

    with scope("loss_terms"):
        usable = lab[...] != 255
        terms = jnp.where(usable, jnp.log(sums[...]) - picks[...], 0.0)
        both = []
        for part in (terms, usable.astype(F32)):
            part = jnp.sum(part, axis=0, keepdims=True)
            both.append(part[:, 0:128] + part[:, 128:256] + part[:, 256:384] + part[:, 384:512])
        sub = lax.broadcasted_iota(jnp.int32, (8, 128), 0)
        loss_rows[pos] = jnp.where(
            sub == 0, jnp.broadcast_to(both[0], (8, 128)), jnp.broadcast_to(both[1], (8, 128)))

    def loss_copy(ref, slot, index, target):
        return pltpu.make_async_remote_copy(
            src_ref=ref.at[slot], dst_ref=ref.at[slot],
            send_sem=loss_send.at[index], recv_sem=loss_recv.at[index],
            device_id=target, device_id_type=MESH,
        )

    def send_row(k, carry):
        loss_copy(loss_rows, pos, 0, {"rows": lax.rem(pos + k, nr)}).start()
        return carry

    lax.fori_loop(1, nr, send_row, 0)

    with scope("scores_out"):
        for k in range(CLASSES):
            for block in range(4):
                out[k, :, block * 128 : (block + 1) * 128] = tall[
                    block, pl.ds(k, 16, stride=36), :
                ].astype(BF16)
        scores_out = local(out, out_hbm.at[0], 15)
        scores_out.start()

    with scope("loss_wait_rows"):
        tiles_wait(loss_rows.at[pl.ds(0, nr - 1)], loss_recv.at[0])
    loss_batch[bat] = functools.reduce(lambda a, b: a + b, [loss_rows[i] for i in range(nr)])

    def send_batch(k, carry):
        loss_copy(loss_batch, bat, 1, {"batch": lax.rem(bat + k, nb)}).start()
        return carry

    lax.fori_loop(1, nb, send_batch, 0)

    with scope("sent_waits"):
        for name in ("t1", "t2", "s", "e", "q", "z"):
            halo_sent(name)
        for layer in range(7):
            tiles_wait(stats.at[layer, pl.ds(0, nr - 1)], stat_send.at[layer])
        tiles_wait(loss_rows.at[pl.ds(0, nr - 1)], loss_send.at[0])
        scores_out.wait()
    with scope("loss_wait_batch"):
        tiles_wait(loss_batch.at[pl.ds(0, nb - 1)], loss_recv.at[1])
    whole = functools.reduce(lambda a, b: a + b, [loss_batch[i] for i in range(nb)])
    whole = jnp.broadcast_to(jnp.sum(whole, axis=1, keepdims=True), (8, 128))
    loss_ref[...] = whole[0:1] / jnp.maximum(whole[1:2], 1.0)
    tiles_wait(loss_batch.at[pl.ds(0, nb - 1)], loss_send.at[1])


def solution(mesh):
    nb, nr = mesh.shape["batch"], mesh.shape["rows"]

    def per_device(xq, x8, x16, x32, labels, fw, iw, gain, shift, cw, cb):
        any_spec = pl.BlockSpec(memory_space=pl.ANY)
        vmem = pl.BlockSpec(memory_space=pltpu.VMEM)
        V = pltpu.VMEM
        dma = pltpu.SemaphoreType.DMA
        logits, loss = pl.pallas_call(
            functools.partial(kernel, nb, nr),
            out_shape=(
                jax.ShapeDtypeStruct((1, CLASSES, 16, 512), BF16),
                jax.ShapeDtypeStruct((1, 128), F32),
            ),
            in_specs=[any_spec] * 11,
            out_specs=(any_spec, vmem),
            scratch_shapes=[
                V((18, 512, 256), BF16), V((10, 256, 256), BF16), V((8, 128, 256), BF16),
                V((8, 64, 256), BF16), V((16, 512), jnp.int32), V((4, 3, 3, 256, 128), BF16),
                V((3, 3, 3, 128, 128), BF16), V((7, 128), F32), V((7, 128), F32),
                V((CLASSES, 128), BF16), V((1, CLASSES), F32),
                V((16, 512, 128), F32), V((8, 256, 128), F32), V((6, 128, 128), F32),
                V((6, 64, 128), F32), V((8, 256, 128), F32), V((6, 128, 128), F32),
                V((8, 256, 128), F32),
                V((6, 128, 128), BF16), V((6, 64, 128), BF16), V((6, 128, 128), BF16),
                V((10, 256, 128), BF16), V((8, 128, 128), BF16), V((10, 256, 128), BF16),
                V((2, 2, 2, 528, 128), F32), V((2, 2, 4, 272, 128), F32),
                V((2, 2, 6, 144, 128), F32), V((2, 2, 6, 80, 128), F32),
                V((128, 128), F32), V((256, 256), BF16), V((256, 512), BF16),
                V((128, 128), F32), V((32, 256), BF16), V((32, 128), F32),
                V((8, 32, 256), F32), V((2, 32, 256), F32), V((10, 32, 512), F32),
                V((16, 512), F32), V((16, 512), F32), V((4, 16 * 36, 128), F32),
                V((CLASSES, 16, 512), BF16),
                V((7, 8, 8, 128), F32), V((7, nr, 8, 128), F32), V((nr, 8, 128), F32),
                V((nb, 8, 128), F32),
                dma((16,)), dma((12,)), dma((12,)), dma((7,)), dma((7,)), dma((2,)), dma((2,)),
            ],
            compiler_params=pltpu.CompilerParams(
                collective_id=0, has_side_effects=True, vmem_limit_bytes=60 * 1024 * 1024
            ),
        )(xq, x8, x16, x32, labels, fw, iw, gain, shift, cw.T, cb.reshape(1, CLASSES))
        return logits, loss[0, 0]

    batch, rows = "batch", "rows"
    return jax.shard_map(
        per_device, mesh=mesh,
        in_specs=(P(batch, rows, None, None),) * 4 + (P(batch, rows, None),) + (P(),) * 6,
        out_specs=(P(batch, None, rows, None), P()),
        check_vma=False,
    )
```

```python
import functools

import jax
import jax.numpy as jnp
from jax import lax
from jax.experimental import pallas as pl
from jax.experimental.pallas import tpu as pltpu
from jax.sharding import PartitionSpec as P

MESH = pl.DeviceIdType.MESH
FLOOR = 0.05
CLASSES = 19
F32 = jnp.float32
BF16 = jnp.bfloat16


def group_total(tile):
    lane = lax.broadcasted_iota(jnp.int32, tile.shape, 1)
    tile = tile + jnp.where(lane % 2 == 0, pltpu.roll(tile, 127, 1), pltpu.roll(tile, 1, 1))
    return tile + jnp.where(lane % 4 < 2, pltpu.roll(tile, 126, 1), pltpu.roll(tile, 2, 1))


def double_matrix(width, out_axis):
    shape = (2 * width, width) if out_axis == 0 else (width, 2 * width)
    out = lax.broadcasted_iota(jnp.int32, shape, out_axis)
    src = lax.broadcasted_iota(jnp.int32, shape, 1 - out_axis)
    half = out // 2
    other = jnp.clip(half + 2 * (out % 2) - 1, 0, width - 1)
    return jnp.where(src == half, 0.75, 0.0) + jnp.where(src == other, 0.25, 0.0)


def kernel(
    nb, nr,
    xq_hbm, x8_hbm, x16_hbm, x32_hbm, lab_hbm, fw_hbm, iw_hbm, gain_hbm, shift_hbm, cw_hbm, cb_hbm,
    out_ref, loss_ref,
    xq, x8, x16, x32, lab, fw, iw, gain, shift, cw, cb,
    yq, y8, y16, y32, y4, y5, y6,
    a16, a32, a5, in4, in5, in6,
    p512, p256, p128, p64,
    u64, u128, u256, cwf, wct, bias,
    zt, ze, z6, zc, sums, picks, tall,
    wq, w8, w16, w32, wi,
    moms, stats, loss_rows, loss_batch,
    local_sem, halo_send, halo_recv, stat_send, stat_recv, loss_send, loss_recv,
):
    pos = lax.axis_index("rows")
    bat = lax.axis_index("batch")
    last = nr - 1
    scope = jax.named_scope

    def local(src, dst, index):
        return pltpu.make_async_copy(src, dst, local_sem.at[index])

    copies = {
        "fw0": local(fw_hbm.at[0], fw.at[0], 2),
        "xqa": local(xq_hbm.at[0, pl.ds(0, 6)], xq.at[pl.ds(1, 6)], 3),
        "x32": local(x32_hbm.at[0], x32.at[pl.ds(3, 2)], 1),
        "x16": local(x16_hbm.at[0], x16.at[pl.ds(2, 4)], 10),
        "fw3": local(fw_hbm.at[3], fw.at[3], 0),
        "xqb": local(xq_hbm.at[0, pl.ds(6, 10)], xq.at[pl.ds(7, 10)], 4),
        "fw2": local(fw_hbm.at[2], fw.at[2], 9),
        "gain": local(gain_hbm, gain, 5),
        "shift": local(shift_hbm, shift, 6),
        "iw": local(iw_hbm, iw, 11),
        "x8": local(x8_hbm.at[0], x8.at[pl.ds(1, 8)], 13),
        "fw1": local(fw_hbm.at[1], fw.at[1], 12),
        "cw": local(cw_hbm, cw, 7),
        "cb": local(cb_hbm, cb, 8),
        "lab": local(lab_hbm.at[0], lab, 14),
    }

    barrier = pltpu.get_barrier_semaphore()

    def greet(axis, peer):
        pl.semaphore_signal(barrier, inc=1, device_id={axis: peer}, device_id_type=MESH)

    with scope("local_start"):
        for copy in copies.values():
            copy.start()
    with scope("greet"):
        for k in sorted(range(1, nr), key=lambda k: -(min(k // 4, 4 - k // 4) + min(k % 4, 4 - k % 4))):
            greet("rows", lax.rem(pos + k, nr))
        for k in range(1, nb):
            greet("batch", lax.rem(bat + k, nb))

    with scope("constants"):
        m64 = double_matrix(64, 0)
        u64[:, 0:64] = 0.75 * m64
        u64[:, 64:128] = 0.25 * m64
        m128 = double_matrix(128, 0)
        u128[:, 0:128] = (0.75 * m128).astype(BF16)
        u128[:, 128:256] = (0.25 * m128).astype(BF16)
        for scratch, width in ((p512, 512), (p256, 256), (p128, 128), (p64, 64)):
            rows = scratch.shape[2]
            scratch[:, :, :, 0:8, :] = jnp.zeros((2, 2, rows, 8, 128), F32)
            scratch[:, :, :, width + 8 : width + 16, :] = jnp.zeros((2, 2, rows, 8, 128), F32)

        @pl.when(pos == 0)
        def _():
            xq[0] = jnp.zeros_like(xq[0])
            x8[0] = jnp.zeros_like(x8[0])
            x16[0:2] = jnp.zeros_like(x16[0:2])
            x32[0:3] = jnp.zeros_like(x32[0:3])

        @pl.when(pos == 1)
        def _():
            x32[0] = jnp.zeros_like(x32[0])

        @pl.when(pos == last)
        def _():
            xq[17] = jnp.zeros_like(xq[17])
            x8[9] = jnp.zeros_like(x8[9])
            x16[6:8] = jnp.zeros_like(x16[6:8])
            x32[5:8] = jnp.zeros_like(x32[5:8])

        @pl.when(pos == last - 1)
        def _():
            x32[7] = jnp.zeros_like(x32[7])

    def remote(src, dst, index, step):
        return pltpu.make_async_remote_copy(
            src_ref=src, dst_ref=dst, send_sem=halo_send.at[index], recv_sem=halo_recv.at[index],
            device_id={"rows": pos + step}, device_id_type=MESH,
        )

    def halos(name, piece=None):
        if name == "t0":
            return (remote(x32.at[pl.ds(4, 1)], x32.at[pl.ds(2, 1)], 12, 1),
                    remote(x32.at[pl.ds(3, 1)], x32.at[pl.ds(5, 1)], 13, -1), 1)
        if name == "t1":
            return (remote(x32.at[pl.ds(3, 1)], x32.at[pl.ds(1, 1)], 0, 1),
                    remote(x32.at[pl.ds(4, 1)], x32.at[pl.ds(6, 1)], 1, -1), 1)
        if name == "t2":
            return (remote(x32.at[pl.ds(4, 1)], x32.at[pl.ds(0, 1)], 2, 2),
                    remote(x32.at[pl.ds(3, 1)], x32.at[pl.ds(7, 1)], 3, -2), 2)
        if name == "s":
            return (remote(x16.at[pl.ds(4, 2)], x16.at[pl.ds(0, 2)], 4, 1),
                    remote(x16.at[pl.ds(2, 2)], x16.at[pl.ds(6, 2)], 5, -1), 1)
        if name == "e":
            return (remote(x8.at[pl.ds(8, 1)], x8.at[pl.ds(0, 1)], 6, 1),
                    remote(x8.at[pl.ds(1, 1)], x8.at[pl.ds(9, 1)], 7, -1), 1)
        if name == "z":
            return (remote(zt.at[7], ze.at[0], 10, 1), remote(zt.at[0], ze.at[1], 11, -1), 1)
        cols = pl.ds(0, 512) if piece is None else pl.ds(piece * 128, 128)
        return (remote(xq.at[16, cols], xq.at[0, cols], 8, 1),
                remote(xq.at[1, cols], xq.at[17, cols], 9, -1), 1)

    def halo_start(name, piece=None):
        down, up, step = halos(name, piece)
        pl.when(pos + step <= last)(down.start)
        pl.when(pos - step >= 0)(up.start)

    def halo_wait(name):
        down, up, step = halos(name)
        pl.when(pos - step >= 0)(down.wait_recv)
        pl.when(pos + step <= last)(up.wait_recv)

    def halo_sent(name):
        down, up, step = halos(name)
        pl.when(pos + step <= last)(down.wait_send)
        pl.when(pos - step >= 0)(up.wait_send)

    def column_sum(values):
        pixels = values.shape[0]
        values = values.reshape(pixels // 64, 8, 8, 128)
        return jnp.sum(jnp.sum(values, axis=0), axis=0)

    def pair_weights(w_ref, out):
        depth = w_ref.shape[2]
        nothing = jnp.zeros((depth, 128), BF16)
        for t in range(4):
            out[t * depth : (t + 1) * depth, 0:128] = w_ref[t, 2] if t < 3 else nothing
            out[t * depth : (t + 1) * depth, 128:256] = w_ref[t - 1, 2] if t > 0 else nothing

    def conv(layer, x_ref, in_off, w_ref, w_pair, y_ref, width, pads):
        def multiply(step):
            rows, _, slot = step
            pad = pads.at[slot % 2]
            joined = rows[1] == rows[0] + 1
            taps = 2 if joined else 3
            lhs = jnp.concatenate(
                [jnp.concatenate([x_ref[in_off + row + dr] for row in rows], axis=0)
                 for dr in range(3)], axis=1)
            rhs = jnp.concatenate(
                [jnp.concatenate([w_ref[dr, dc] for dc in range(taps)], axis=1) for dr in range(3)],
                axis=0)
            part = jnp.dot(lhs, rhs, preferred_element_type=F32)
            for i, row in enumerate(rows):
                here = slice(i * width, (i + 1) * width)
                pad[0, i, 8 : 8 + width, :] = part[here, 0:128]
                y_ref[row] = part[here, 128:256]
                if not joined:
                    pad[1, i, 8 : 8 + width, :] = part[here, 256:384]
            if joined:
                lhs = jnp.concatenate(
                    [jnp.concatenate([x_ref[in_off + row + t] for row in rows[::2]], axis=0)
                     for t in range(4)], axis=1)
                part = jnp.dot(lhs, w_pair[...], preferred_element_type=F32)
                for i in range(len(rows)):
                    here = slice((i // 2) * width, (i // 2 + 1) * width)
                    side = slice((i % 2) * 128, (i % 2) * 128 + 128)
                    pad[1, i, 8 : 8 + width, :] = part[here, side]

        def settle(step):
            rows, own, slot = step
            pad = pads.at[slot % 2]
            for i, row in enumerate(rows):
                y_ref[row] = y_ref[row] + pad[0, i, 7 : 7 + width, :] + pad[1, i, 9 : 9 + width, :]
            if not own:
                return
            count = len(own) * width
            total = sum(column_sum(y_ref[row]) for row in own)
            mean = jnp.sum(total, axis=0, keepdims=True) * (1.0 / count)
            square = jnp.zeros((8, 128), F32)
            for row in own:
                off = y_ref[row] - mean
                square = square + column_sum(off * off)
            moms[layer, slot, 0:1, :] = mean
            moms[layer, slot, 1:2, :] = jnp.sum(square, axis=0, keepdims=True)

        return multiply, settle

    def run(pieces, steps, before=(), keep=False):
        multiply, settle = pieces
        waiting = list(before)
        for step in steps:
            multiply(step)
            for old in waiting:
                settle(old)
            waiting = [step]
        if keep:
            return waiting
        for old in waiting:
            settle(old)
        return []

    def moments(layer, slots, pixels):
        tiles = [moms[layer, i] for i in range(slots)]
        total = functools.reduce(lambda a, b: a + b, tiles)
        channel = total[0:1] * (1.0 / slots)
        share = pixels // slots
        square = total[1:2]
        for tile in tiles:
            square = square + share * (tile[0:1] - channel) * (tile[0:1] - channel)
        channel = jnp.broadcast_to(channel, (8, 128))
        square = jnp.broadcast_to(square, (8, 128))
        mean = group_total(channel) * 0.25
        square = group_total(square + pixels * (channel - mean) * (channel - mean))
        sub = lax.broadcasted_iota(jnp.int32, (8, 128), 0)
        stats[layer, pos] = jnp.where(sub == 0, mean, square)[0:2]

        def send(k, carry):
            stat_copy(layer, lax.rem(pos + k, nr)).start()
            return carry

        lax.fori_loop(1, nr, send, 0)

    def stat_copy(layer, peer):
        return pltpu.make_async_remote_copy(
            src_ref=stats.at[layer, pos], dst_ref=stats.at[layer, pos],
            send_sem=stat_send.at[layer], recv_sem=stat_recv.at[layer],
            device_id={"rows": peer}, device_id_type=MESH,
        )

    def tiles_wait(ref, sem):
        pltpu.make_async_copy(ref, ref, sem).wait()

    def scales(layer, pixels):
        local_count = 4 * pixels
        with scope(f"stat_wait{layer}"):
            tiles_wait(stats.at[layer, pl.ds(0, nr - 1)], stat_recv.at[layer])
        every = [stats[layer, i] for i in range(nr)]
        total = functools.reduce(lambda a, b: a + b, every)
        mean = total[0:1] * (1.0 / nr)
        spread = [(tile[0:1] - mean) * (tile[0:1] - mean) for tile in every]
        square = total[1:2] + local_count * functools.reduce(lambda a, b: a + b, spread)
        var = square * (1.0 / (nr * local_count))
        factor = gain[pl.ds(layer, 1), :] * lax.rsqrt(var + FLOOR)
        return mean, factor, shift[pl.ds(layer, 1), :]

    def activate(values, scale):
        mean, factor, offset = scale
        return jnp.maximum((values - mean) * factor + offset, 0.0).astype(BF16)

    def normalize(y_ref, a_ref, scale, rows, top, bottom):
        for r in range(rows):
            a_ref[r] = activate(y_ref[r], scale)

        @pl.when(pos == 0)
        def _():
            a_ref[top] = a_ref[top + 1]

        @pl.when(pos == last)
        def _():
            a_ref[bottom] = a_ref[bottom - 1]

    def double(a_ref, u_ref, in_ref, pairs):
        top_row = a_ref.shape[0] - 1
        end = in_ref.shape[0]
        for k, j in pairs:
            mid = a_ref[k]
            rhs = jnp.concatenate(
                [jnp.concatenate([mid, mid], axis=1),
                 jnp.concatenate([a_ref[max(k - 1, 0)], a_ref[min(k + 1, top_row)]], axis=1)],
                axis=0)
            both = jnp.dot(u_ref[...].astype(BF16), rhs, preferred_element_type=F32).astype(BF16)
            if j >= 0:
                in_ref[j] = both[:, 0:128]
            if j + 1 < end:
                in_ref[j + 1] = both[:, 128:256]

    def clear_outside(in_ref, top_rows, bottom_row):
        @pl.when(pos == 0)
        def _():
            in_ref[0:top_rows] = jnp.zeros_like(in_ref[0:top_rows])

        @pl.when(pos == last)
        def _():
            rest = in_ref.shape[0] - bottom_row
            in_ref[bottom_row:] = jnp.zeros((rest,) + in_ref.shape[1:], BF16)

    nt = (((1,), (1,)), ((), ()))

    quarter = conv(0, xq, 0, fw.at[0], wq, yq, 512, p512)

    def band(*firsts):
        return [((r, r + 1),) * 2 + (r // 2,) for r in firsts]

    with scope("q_wait_a"):
        copies["fw0"].wait()
        copies["xqa"].wait()
    with scope("q_pre"):
        pair_weights(fw.at[0], wq)
        late = run(quarter, band(1), keep=True)

    with scope("barrier"):
        copies["x32"].wait()
        copies["x16"].wait()
        pl.semaphore_wait(barrier, nr - 1 + nb - 1)
    with scope("send_ts"):
        halo_start("t0")
        halo_start("s")
        halo_start("t1")

    with scope("q_wait_b"):
        copies["xqb"].wait()
    with scope("q_a"):
        late = run(quarter, band(3, 5, 7, 9), late, keep=True)

    with scope("class_consts"):
        copies["fw3"].wait()
        copies["cw"].wait()
        copies["cb"].wait()
        pair_weights(fw.at[3], w32)
        u256[...] = double_matrix(256, 1).astype(BF16)
        cwf[...] = jnp.zeros_like(cwf)
        cwf[0:CLASSES, :] = cw[...].astype(F32)
        wct[:, 0:128] = cwf[0:32, :].astype(BF16)
        wct[:, 128:256] = cwf[0:32, :].astype(BF16)
        cwf[...] = jnp.zeros_like(cwf)
        cwf[0:1, 0:CLASSES] = cb[...]
        bias[...] = jnp.broadcast_to(jnp.transpose(cwf[...])[0:32, 0:1], (32, 128))

    level3 = conv(3, x32, 0, fw.at[3], w32, y32, 64, p64)
    with scope("t_wait"):
        halo_wait("t0")
    with scope("l3"):
        run(level3, [((2, 3), (2, 3), 0)])
        moments(3, 1, 2 * 64)
    copies["x8"].wait()
    halo_start("t2")
    halo_start("e")

    with scope("q_b"):
        late = run(quarter, band(11, 13), late, keep=True)
        copies["fw2"].wait()
        copies["fw1"].wait()
        copies["iw"].wait()
        pair_weights(fw.at[2], w16)
        pair_weights(fw.at[1], w8)
        for i in range(3):
            pair_weights(iw.at[i], wi.at[i])

    six = tuple(range(6))
    mid = (1, 2, 3, 4)
    with scope("s_wait"):
        halo_wait("s")
    with scope("l2"):
        run(conv(2, x16, 0, fw.at[2], w16, y16, 128, p128), [(six, mid, 0)])
        moments(2, 1, 4 * 128)
    halo_start("q", 0)

    with scope("t12_wait"):
        halo_wait("t1")
        halo_wait("t2")
        copies["gain"].wait()
        copies["shift"].wait()
    with scope("l3_ext"):
        run(level3, [((0, 1, 4, 5), (), 1)])
    scale3 = scales(3, 2 * 64)
    level5 = conv(5, in5, 1, iw.at[1], wi.at[1], y5, 128, p128)
    with scope("l5"):
        normalize(y32, a32, scale3, 6, 1, 4)
        double(a32, u64, in5, [(k, 2 * k) for k in range(6)])
        clear_outside(in5, 4, 8)
        run(level5, [((2, 3, 4, 5),) * 2 + (0,)])
        moments(5, 1, 4 * 128)
    halo_start("q", 1)
    halo_start("q", 2)
    with scope("l5_ext"):
        run(level5, [((0, 1, 6, 7), (), 1)])

    eight = [((0, 1, 2, 3),) * 2 + (0,), ((4, 5, 6, 7),) * 2 + (1,)]
    with scope("e_wait"):
        halo_wait("e")
    with scope("l1"):
        run(conv(1, x8, 0, fw.at[1], w8, y8, 256, p256), eight)
        moments(1, 2, 8 * 256)
    halo_start("q", 3)

    scale2 = scales(2, 4 * 128)
    with scope("l4"):
        normalize(y16, a16, scale2, 6, 0, 5)
        double(a16, u128, in4, [(k, 2 * k - 1) for k in range(6)])
        clear_outside(in4, 1, 9)
        run(conv(4, in4, 0, iw.at[0], wi.at[0], y4, 256, p256), eight)
        moments(4, 2, 8 * 256)

    scale5 = scales(5, 4 * 128)
    level6 = conv(6, in6, 0, iw.at[2], wi.at[2], y6, 256, p256)
    with scope("l6"):
        normalize(y5, a5, scale5, 8, 1, 6)
        double(a5, u128, in6, [(k, 2 * k - 2) for k in range(1, 7)])
        clear_outside(in6, 2, 10)
        run(level6, [((1, 2, 3, 4),) * 2 + (0,), ((5, 6, 7, 8),) * 2 + (1,)])
        moments(6, 2, 8 * 256)

    with scope("q_wait_e"):
        halo_wait("q")
    with scope("q_e"):
        run(quarter, [((0, 15), (0, 15), 7)], late)
        moments(0, 8, 16 * 512)
        copies["lab"].wait()

    with scope("l6_ext"):
        run(level6, [((0, 9), (), 2)])
    scale1 = scales(1, 8 * 256)
    scale4 = scales(4, 8 * 256)
    with scope("z14"):
        for half in range(2):
            act = jnp.concatenate(
                [jnp.concatenate([activate(y4[r], scale4), activate(y8[r], scale1)], axis=1)
                 for r in range(half * 4, half * 4 + 4)], axis=0)
            part = lax.dot_general(wct[...], act, nt, preferred_element_type=F32)
            for i in range(4):
                zt[half * 4 + i] = part[:, i * 256 : (i + 1) * 256]
    halo_start("z")
    scale6 = scales(6, 8 * 256)
    with scope("z6"):
        for half in range(2):
            act = jnp.concatenate(
                [activate(y6[r], scale6) for r in range(half * 5, half * 5 + 5)], axis=0)
            part = lax.dot_general(wct[:, 0:128], act, nt, preferred_element_type=F32)
            for i in range(5):
                z6[half * 5 + i] = part[:, i * 256 : (i + 1) * 256]

    def widen(flat):
        high = flat.astype(BF16)
        low = (flat - high.astype(F32)).astype(BF16)
        return (jnp.dot(high, u256[...], preferred_element_type=F32)
                + jnp.dot(low, u256[...], preferred_element_type=F32))

    with scope("widen"):
        zc[1:9] = widen((zt[...] + z6[1:9]).reshape(256, 256)).reshape(8, 32, 512)

        @pl.when(pos == 0)
        def _():
            ze[0] = zt[0]
            z6[0] = z6[1]

        @pl.when(pos == last)
        def _():
            ze[1] = zt[7]
            z6[9] = z6[8]

    scale0 = scales(0, 16 * 512)

    def finish(rows):
        act = jnp.concatenate([activate(yq[r], scale0) for r in rows], axis=0)
        main = lax.dot_general(wct[:, 0:128], act, nt, preferred_element_type=F32)
        kind = lax.broadcasted_iota(jnp.int32, (32, 512), 0)
        offset = jnp.concatenate([bias[...]] * 4, axis=1)
        for i, r in enumerate(rows):
            half = r // 2
            near = half + 2 * (r % 2)
            score = (main[:, i * 512 : (i + 1) * 512] + offset
                     + 0.75 * zc[half + 1] + 0.25 * zc[near])
            grown = jnp.where(kind < CLASSES, jnp.exp(score), 0.0)
            sums[r : r + 1, :] = jnp.sum(grown, axis=0, keepdims=True)
            marks = jnp.broadcast_to(lab[r : r + 1, :], (32, 512))
            picks[r : r + 1, :] = jnp.sum(
                jnp.where(kind == marks, score, 0.0), axis=0, keepdims=True)
            for block in range(4):
                tall[block, r * 36 : r * 36 + 32, :] = score[:, block * 128 : (block + 1) * 128]

    with scope("finish"):
        for r in range(1, 15, 2):
            finish((r, r + 1))
    with scope("z_wait"):
        halo_wait("z")
    with scope("finish_edge"):
        edges = widen(jnp.concatenate([ze[0] + z6[0], ze[1] + z6[9]], axis=0))
        zc[0] = edges[0:32]
        zc[9] = edges[32:64]
        finish((0, 15))

    with scope("loss_terms"):
        usable = lab[...] != 255
        terms = jnp.where(usable, jnp.log(sums[...]) - picks[...], 0.0)
        both = []
        for part in (terms, usable.astype(F32)):
            part = jnp.sum(part, axis=0, keepdims=True)
            both.append(part[:, 0:128] + part[:, 128:256] + part[:, 256:384] + part[:, 384:512])
        sub = lax.broadcasted_iota(jnp.int32, (8, 128), 0)
        loss_rows[pos] = jnp.where(
            sub == 0, jnp.broadcast_to(both[0], (8, 128)), jnp.broadcast_to(both[1], (8, 128)))[0:2]

    def loss_copy(ref, slot, index, target):
        return pltpu.make_async_remote_copy(
            src_ref=ref.at[slot], dst_ref=ref.at[slot],
            send_sem=loss_send.at[index], recv_sem=loss_recv.at[index],
            device_id=target, device_id_type=MESH,
        )

    def send_row(k, carry):
        loss_copy(loss_rows, pos, 0, {"rows": lax.rem(pos + k, nr)}).start()
        return carry

    lax.fori_loop(1, nr, send_row, 0)

    with scope("scores_out"):
        for k in range(CLASSES):
            for block in range(4):
                out_ref[0, k, :, block * 128 : (block + 1) * 128] = tall[
                    block, pl.ds(k, 16, stride=36), :
                ].astype(BF16)

    with scope("loss_wait_rows"):
        tiles_wait(loss_rows.at[pl.ds(0, nr - 1)], loss_recv.at[0])
    loss_batch[bat] = functools.reduce(lambda a, b: a + b, [loss_rows[i] for i in range(nr)])

    def send_batch(k, carry):
        loss_copy(loss_batch, bat, 1, {"batch": lax.rem(bat + k, nb)}).start()
        return carry

    lax.fori_loop(1, nb, send_batch, 0)

    with scope("sent_waits"):
        for name in ("t0", "t1", "t2", "s", "e", "q", "z"):
            halo_sent(name)
        for layer in range(7):
            tiles_wait(stats.at[layer, pl.ds(0, nr - 1)], stat_send.at[layer])
        tiles_wait(loss_rows.at[pl.ds(0, nr - 1)], loss_send.at[0])
    with scope("loss_wait_batch"):
        tiles_wait(loss_batch.at[pl.ds(0, nb - 1)], loss_recv.at[1])
    whole = functools.reduce(lambda a, b: a + b, [loss_batch[i] for i in range(nb)])
    whole = jnp.broadcast_to(jnp.sum(whole, axis=1, keepdims=True), (2, 128))
    loss_ref[...] = whole[0:1] / jnp.maximum(whole[1:2], 1.0)
    tiles_wait(loss_batch.at[pl.ds(0, nb - 1)], loss_send.at[1])


def solution(mesh):
    nb, nr = mesh.shape["batch"], mesh.shape["rows"]

    def per_device(xq, x8, x16, x32, labels, fw, iw, gain, shift, cw, cb):
        any_spec = pl.BlockSpec(memory_space=pl.ANY)
        vmem = pl.BlockSpec(memory_space=pltpu.VMEM)
        V = pltpu.VMEM
        dma = pltpu.SemaphoreType.DMA
        logits, loss = pl.pallas_call(
            functools.partial(kernel, nb, nr),
            out_shape=(
                V((1, CLASSES, 16, 512), BF16),
                V((1, 128), F32),
            ),
            in_specs=[any_spec] * 11,
            out_specs=(vmem, vmem),
            scratch_shapes=[
                V((18, 512, 256), BF16), V((10, 256, 256), BF16), V((8, 128, 256), BF16),
                V((8, 64, 256), BF16), V((16, 512), jnp.int32), V((4, 3, 3, 256, 128), BF16),
                V((3, 3, 3, 128, 128), BF16), V((7, 128), F32), V((7, 128), F32),
                V((CLASSES, 128), BF16), V((1, CLASSES), F32),
                V((16, 512, 128), F32), V((8, 256, 128), F32), V((6, 128, 128), F32),
                V((6, 64, 128), F32), V((8, 256, 128), F32), V((8, 128, 128), F32),
                V((10, 256, 128), F32),
                V((6, 128, 128), BF16), V((6, 64, 128), BF16), V((8, 128, 128), BF16),
                V((10, 256, 128), BF16), V((12, 128, 128), BF16), V((12, 256, 128), BF16),
                V((2, 2, 2, 528, 128), F32), V((2, 2, 4, 272, 128), F32),
                V((2, 2, 6, 144, 128), F32), V((2, 2, 6, 80, 128), F32),
                V((128, 128), F32), V((256, 256), BF16), V((256, 512), BF16),
                V((128, 128), F32), V((32, 256), BF16), V((32, 128), F32),
                V((8, 32, 256), F32), V((2, 32, 256), F32), V((10, 32, 256), F32),
                V((10, 32, 512), F32),
                V((16, 512), F32), V((16, 512), F32), V((4, 16 * 36, 128), F32),
                V((1024, 256), BF16), V((1024, 256), BF16), V((1024, 256), BF16),
                V((1024, 256), BF16), V((3, 512, 256), BF16),
                V((7, 8, 8, 128), F32), V((7, nr, 2, 128), F32), V((nr, 2, 128), F32),
                V((nb, 2, 128), F32),
                dma((15,)), dma((14,)), dma((14,)), dma((7,)), dma((7,)), dma((2,)), dma((2,)),
            ],
            compiler_params=pltpu.CompilerParams(
                collective_id=0, has_side_effects=True, vmem_limit_bytes=60 * 1024 * 1024
            ),
        )(xq, x8, x16, x32, labels, fw, iw, gain, shift, cw.T, cb.reshape(1, CLASSES))
        return logits, loss[0, 0]

    batch, rows = "batch", "rows"
    return jax.shard_map(
        per_device, mesh=mesh,
        in_specs=(P(batch, rows, None, None),) * 4 + (P(batch, rows, None),) + (P(),) * 6,
        out_specs=(P(batch, None, rows, None), P()),
        check_vma=False,
    )
```

```python
import functools

import jax
import jax.numpy as jnp
from jax import lax
from jax.experimental import pallas as pl
from jax.experimental.pallas import tpu as pltpu
from jax.sharding import PartitionSpec as P

MESH = pl.DeviceIdType.MESH
FLOOR = 0.05
CLASSES = 19
F32 = jnp.float32
BF16 = jnp.bfloat16


def group_moments(mean, square, count):
    lane = lax.broadcasted_iota(jnp.int32, mean.shape, 1)
    for bit in (1, 2):
        low = lane % (2 * bit) < bit

        def other(tile):
            return jnp.where(low, pltpu.roll(tile, 128 - bit, 1), pltpu.roll(tile, bit, 1))

        off = mean - other(mean)
        square = square + other(square) + (count * bit * 0.5) * off * off
        mean = 0.5 * (mean + other(mean))
    return mean, square


def tree_sum(items):
    while len(items) > 1:
        items = [sum(items[i : i + 2][1:], items[i]) for i in range(0, len(items), 2)]
    return items[0]


def double_matrix(width, out_axis):
    shape = (2 * width, width) if out_axis == 0 else (width, 2 * width)
    out = lax.broadcasted_iota(jnp.int32, shape, out_axis)
    src = lax.broadcasted_iota(jnp.int32, shape, 1 - out_axis)
    half = out // 2
    other = jnp.clip(half + 2 * (out % 2) - 1, 0, width - 1)
    return jnp.where(src == half, 0.75, 0.0) + jnp.where(src == other, 0.25, 0.0)


def kernel(
    nb, nr,
    xq_hbm, x8_hbm, x16_hbm, x32_hbm, lab_hbm, fw_hbm, iw_hbm, gain_hbm, shift_hbm, cw_hbm, cb_hbm,
    out_ref, loss_ref,
    xq, x8, x16, x32, lab, fw, iw, gain, shift, cw, cb,
    yq, y8, y16, y32, y4, y5, y6,
    a16, a32, a5, in4, in5, in6,
    p512, p256, p128, p64,
    u64, u128, u256, cwf, wct, two, bias,
    zt, ze, z6, zc, sums, picks, tall,
    wq, w8, w16, w32, wi,
    moms, stats, loss_rows, loss_batch,
    local_sem, halo_send, halo_recv, stat_send, stat_recv, loss_send, loss_recv,
):
    pos = lax.axis_index("rows")
    bat = lax.axis_index("batch")
    last = nr - 1
    scope = jax.named_scope

    def local(src, dst, index):
        return pltpu.make_async_copy(src, dst, local_sem.at[index])

    copies = {
        "fw0": local(fw_hbm.at[0], fw.at[0], 2),
        "xqa": local(xq_hbm.at[0, pl.ds(0, 4)], xq.at[pl.ds(1, 4)], 3),
        "x32": local(x32_hbm.at[0], x32.at[pl.ds(3, 2)], 1),
        "x16": local(x16_hbm.at[0], x16.at[pl.ds(2, 4)], 10),
        "fw3": local(fw_hbm.at[3], fw.at[3], 0),
        "xqb": local(xq_hbm.at[0, pl.ds(4, 12)], xq.at[pl.ds(5, 12)], 4),
        "fw2": local(fw_hbm.at[2], fw.at[2], 9),
        "gain": local(gain_hbm, gain, 5),
        "shift": local(shift_hbm, shift, 6),
        "iw": local(iw_hbm, iw, 11),
        "x8": local(x8_hbm.at[0], x8.at[pl.ds(1, 8)], 13),
        "fw1": local(fw_hbm.at[1], fw.at[1], 12),
        "cw": local(cw_hbm, cw, 7),
        "cb": local(cb_hbm, cb, 8),
        "lab": local(lab_hbm.at[0], lab, 14),
    }

    barrier = pltpu.get_barrier_semaphore()

    far = sorted(
        [(dz, dy) for dz in range(4) for dy in range(4) if dz or dy],
        key=lambda d: -(min(d[0], 4 - d[0]) + min(d[1], 4 - d[1])))

    def row_peers():
        return [lax.rem(pos // 4 + dz, 4) * 4 + lax.rem(lax.rem(pos, 4) + dy, 4) for dz, dy in far]

    def batch_peers():
        return [lax.rem(bat + k, nb) for k in sorted(range(1, nb), key=lambda k: -min(k, nb - k))]

    def greet(axis, peer):
        pl.semaphore_signal(barrier, inc=1, device_id={axis: peer}, device_id_type=MESH)

    with scope("local_start"):
        for copy in copies.values():
            copy.start()
    with scope("greet"):
        for peer in row_peers():
            greet("rows", peer)
        for peer in batch_peers():
            greet("batch", peer)

    with scope("constants"):
        m64 = double_matrix(64, 0)
        u64[:, 0:64] = 0.75 * m64
        u64[:, 64:128] = 0.25 * m64
        m128 = double_matrix(128, 0)
        u128[:, 0:128] = (0.75 * m128).astype(BF16)
        u128[:, 128:256] = (0.25 * m128).astype(BF16)
        for scratch, width in ((p512, 512), (p256, 256), (p128, 128), (p64, 64)):
            rows = scratch.shape[2]
            scratch[:, :, :, 0:8, :] = jnp.zeros((2, 2, rows, 8, 128), F32)
            scratch[:, :, :, width + 8 : width + 16, :] = jnp.zeros((2, 2, rows, 8, 128), F32)

        @pl.when(pos == 0)
        def _():
            xq[0] = jnp.zeros_like(xq[0])
            x8[0] = jnp.zeros_like(x8[0])
            x16[0:2] = jnp.zeros_like(x16[0:2])
            x32[0:3] = jnp.zeros_like(x32[0:3])

        @pl.when(pos == 1)
        def _():
            x32[0] = jnp.zeros_like(x32[0])

        @pl.when(pos == last)
        def _():
            xq[17] = jnp.zeros_like(xq[17])
            x8[9] = jnp.zeros_like(x8[9])
            x16[6:8] = jnp.zeros_like(x16[6:8])
            x32[5:8] = jnp.zeros_like(x32[5:8])

        @pl.when(pos == last - 1)
        def _():
            x32[7] = jnp.zeros_like(x32[7])

    def remote(src, dst, index, step):
        return pltpu.make_async_remote_copy(
            src_ref=src, dst_ref=dst, send_sem=halo_send.at[index], recv_sem=halo_recv.at[index],
            device_id={"rows": pos + step}, device_id_type=MESH,
        )

    def halos(name, piece=None):
        if name == "t0":
            return (remote(x32.at[pl.ds(4, 1)], x32.at[pl.ds(2, 1)], 12, 1),
                    remote(x32.at[pl.ds(3, 1)], x32.at[pl.ds(5, 1)], 13, -1), 1)
        if name == "t1":
            return (remote(x32.at[pl.ds(3, 1)], x32.at[pl.ds(1, 1)], 0, 1),
                    remote(x32.at[pl.ds(4, 1)], x32.at[pl.ds(6, 1)], 1, -1), 1)
        if name == "t2":
            return (remote(x32.at[pl.ds(4, 1)], x32.at[pl.ds(0, 1)], 2, 2),
                    remote(x32.at[pl.ds(3, 1)], x32.at[pl.ds(7, 1)], 3, -2), 2)
        if name == "s0":
            return (remote(x16.at[pl.ds(5, 1)], x16.at[pl.ds(1, 1)], 4, 1),
                    remote(x16.at[pl.ds(2, 1)], x16.at[pl.ds(6, 1)], 5, -1), 1)
        if name == "s1":
            return (remote(x16.at[pl.ds(4, 1)], x16.at[pl.ds(0, 1)], 14, 1),
                    remote(x16.at[pl.ds(3, 1)], x16.at[pl.ds(7, 1)], 15, -1), 1)
        if name == "e":
            return (remote(x8.at[pl.ds(8, 1)], x8.at[pl.ds(0, 1)], 6, 1),
                    remote(x8.at[pl.ds(1, 1)], x8.at[pl.ds(9, 1)], 7, -1), 1)
        if name == "z":
            return (remote(zt.at[7], ze.at[0], 10, 1), remote(zt.at[0], ze.at[1], 11, -1), 1)
        cols = pl.ds(0, 512) if piece is None else pl.ds(piece * 128, 128)
        return (remote(xq.at[16, cols], xq.at[0, cols], 8, 1),
                remote(xq.at[1, cols], xq.at[17, cols], 9, -1), 1)

    def halo_start(name, piece=None):
        down, up, step = halos(name, piece)
        pl.when(pos + step <= last)(down.start)
        pl.when(pos - step >= 0)(up.start)

    def halo_wait(name):
        down, up, step = halos(name)
        pl.when(pos - step >= 0)(down.wait_recv)
        pl.when(pos + step <= last)(up.wait_recv)

    def halo_sent(name):
        down, up, step = halos(name)
        pl.when(pos + step <= last)(down.wait_send)
        pl.when(pos - step >= 0)(up.wait_send)

    def column_sum(values):
        pixels = values.shape[0]
        values = values.reshape(pixels // 64, 8, 8, 128)
        return jnp.sum(jnp.sum(values, axis=0), axis=0)

    def pair_weights(w_ref, out):
        depth = w_ref.shape[2]
        nothing = jnp.zeros((depth, 128), BF16)
        for t in range(4):
            out[t * depth : (t + 1) * depth, 0:128] = w_ref[t, 2] if t < 3 else nothing
            out[t * depth : (t + 1) * depth, 128:256] = w_ref[t - 1, 2] if t > 0 else nothing

    def conv(layer, x_ref, in_off, w_ref, w_pair, y_ref, width, pads):
        def multiply(step):
            rows, _, slot = step
            pad = pads.at[slot % 2]
            joined = rows[1] == rows[0] + 1
            taps = 2 if joined else 3
            lhs = jnp.concatenate(
                [jnp.concatenate([x_ref[in_off + row + dr] for row in rows], axis=0)
                 for dr in range(3)], axis=1)
            rhs = jnp.concatenate(
                [jnp.concatenate([w_ref[dr, dc] for dc in range(taps)], axis=1) for dr in range(3)],
                axis=0)
            part = jnp.dot(lhs, rhs, preferred_element_type=F32)
            for i, row in enumerate(rows):
                here = slice(i * width, (i + 1) * width)
                pad[0, i, 8 : 8 + width, :] = part[here, 0:128]
                y_ref[row] = part[here, 128:256]
                if not joined:
                    pad[1, i, 8 : 8 + width, :] = part[here, 256:384]
            if joined:
                lhs = jnp.concatenate(
                    [jnp.concatenate([x_ref[in_off + row + t] for row in rows[::2]], axis=0)
                     for t in range(4)], axis=1)
                part = jnp.dot(lhs, w_pair[...], preferred_element_type=F32)
                for i in range(len(rows)):
                    here = slice((i // 2) * width, (i // 2 + 1) * width)
                    side = slice((i % 2) * 128, (i % 2) * 128 + 128)
                    pad[1, i, 8 : 8 + width, :] = part[here, side]

        def settle(step):
            rows, own, slot = step
            pad = pads.at[slot % 2]
            for i, row in enumerate(rows):
                y_ref[row] = y_ref[row] + pad[0, i, 7 : 7 + width, :] + pad[1, i, 9 : 9 + width, :]
            if not own:
                return
            count = len(own) * width
            total = sum(column_sum(y_ref[row]) for row in own)
            mean = jnp.sum(total, axis=0, keepdims=True) * (1.0 / count)
            square = jnp.zeros((8, 128), F32)
            for row in own:
                off = y_ref[row] - mean
                square = square + column_sum(off * off)
            moms[layer, slot, 0:1, :] = mean
            moms[layer, slot, 1:2, :] = jnp.sum(square, axis=0, keepdims=True)

        return multiply, settle

    def run(pieces, steps, before=(), keep=False):
        multiply, settle = pieces
        waiting = list(before)
        for step in steps:
            multiply(step)
            for old in waiting:
                old()
            waiting = [functools.partial(settle, step)]
        if keep:
            return waiting
        for old in waiting:
            old()
        return []

    def moments(layer, counts):
        pixels = sum(counts)
        tiles = [moms[layer, i] for i in range(len(counts))]
        channel = tree_sum([tile[0:1] * (n / pixels) for tile, n in zip(tiles, counts)])
        off = [tile[0:1] - channel for tile in tiles]
        square = tree_sum([tile[1:2] + n * (one * one) for tile, n, one in zip(tiles, counts, off)])
        mean, square = group_moments(
            jnp.broadcast_to(channel, (8, 128)), jnp.broadcast_to(square, (8, 128)), pixels)
        sub = lax.broadcasted_iota(jnp.int32, (8, 128), 0)
        stats[layer, pos] = jnp.where(sub == 0, mean, square)[0:2]

        for peer in row_peers():
            stat_copy(layer, peer).start()

    def stat_copy(layer, peer):
        return pltpu.make_async_remote_copy(
            src_ref=stats.at[layer, pos], dst_ref=stats.at[layer, pos],
            send_sem=stat_send.at[layer], recv_sem=stat_recv.at[layer],
            device_id={"rows": peer}, device_id_type=MESH,
        )

    def tiles_wait(ref, sem):
        pltpu.make_async_copy(ref, ref, sem).wait()

    def scales(layer, pixels):
        local_count = 4 * pixels
        with scope(f"stat_wait{layer}"):
            tiles_wait(stats.at[layer, pl.ds(0, nr - 1)], stat_recv.at[layer])
        every = [stats[layer, i] for i in range(nr)]
        total = tree_sum(every)
        mean = total[0:1] * (1.0 / nr)
        off = [tile[0:1] - mean for tile in every]
        square = total[1:2] + local_count * tree_sum([one * one for one in off])
        var = square * (1.0 / (nr * local_count))
        factor = gain[pl.ds(layer, 1), :] * lax.rsqrt(var + FLOOR)
        return factor, shift[pl.ds(layer, 1), :] - mean * factor

    def active(values, scale):
        return jnp.maximum(values * scale[0] + scale[1], 0.0)

    def activate(values, scale):
        return active(values, scale).astype(BF16)

    at_top = jnp.where(pos == 0, 1.0, 0.0).astype(F32)
    at_end = jnp.where(pos == last, 1.0, 0.0).astype(F32)

    def normalize(y_ref, a_ref, scale, rows, top, bottom):
        for r in range(rows):
            value = active(y_ref[r], scale)
            if r == top:
                value = at_top * active(y_ref[r + 1], scale) + (1.0 - at_top) * value
            if r == bottom:
                value = at_end * active(y_ref[r - 1], scale) + (1.0 - at_end) * value
            a_ref[r] = value.astype(BF16)

    def double(a_ref, u_ref, in_ref, pairs, top_rows, bottom_row):
        top_row = a_ref.shape[0] - 1
        for k, j in pairs:
            mid = a_ref[k]
            rhs = jnp.concatenate(
                [jnp.concatenate([mid, mid], axis=1),
                 jnp.concatenate([a_ref[max(k - 1, 0)], a_ref[min(k + 1, top_row)]], axis=1)],
                axis=0)
            both = jnp.dot(u_ref[...].astype(BF16), rhs, preferred_element_type=F32)
            for row, value in ((j, both[:, 0:128]), (j + 1, both[:, 128:256])):
                if 0 <= row < in_ref.shape[0]:
                    if row < top_rows:
                        value = (1.0 - at_top) * value
                    if row >= bottom_row:
                        value = (1.0 - at_end) * value
                    in_ref[row] = value.astype(BF16)

    nt = (((1,), (1,)), ((), ()))

    quarter = conv(0, xq, 0, fw.at[0], wq, yq, 512, p512)

    def band(*firsts):
        return [((r, r + 1),) * 2 + (r // 2,) for r in firsts]

    def edge_rows(taps, fresh):
        pad = p512.at[1]
        for i, row in enumerate((0, 15)):
            lhs = jnp.concatenate([xq[row + dr] for dr in taps[i]], axis=1)
            rhs = jnp.concatenate(
                [jnp.concatenate([fw[0, dr, dc] for dc in range(3)], axis=1) for dr in taps[i]],
                axis=0)
            part = jnp.dot(lhs, rhs, preferred_element_type=F32)
            pad[0, i, 8:520, :] = part[:, 0:128]
            pad[1, i, 8:520, :] = part[:, 256:384]
            yq[row] = part[:, 128:256] if fresh else yq[row] + part[:, 128:256]

    with scope("q_wait_a"):
        copies["fw0"].wait()
        copies["xqa"].wait()
    with scope("q_pre"):
        pair_weights(fw.at[0], wq)
        late = run(quarter, band(1), keep=True)

    with scope("barrier"):
        copies["x32"].wait()
        copies["x16"].wait()
        pl.semaphore_wait(barrier, nr - 1 + nb - 1)
    with scope("send_ts"):
        halo_start("t0")
        halo_start("s0")
        halo_start("t1")
        halo_start("t2")

    with scope("q_wait_b"):
        copies["xqb"].wait()
    with scope("q_a"):
        late = run(quarter, band(3, 5, 7, 9), late, keep=True)

    with scope("class_consts"):
        copies["fw3"].wait()
        copies["cw"].wait()
        copies["cb"].wait()
        pair_weights(fw.at[3], w32)
        for name in ("fw2", "fw1", "iw"):
            copies[name].wait()
        pair_weights(fw.at[2], w16)
        pair_weights(fw.at[1], w8)
        for i in range(3):
            pair_weights(iw.at[i], wi.at[i])
        u256[...] = double_matrix(256, 1).astype(BF16)
        cwf[...] = jnp.zeros_like(cwf)
        cwf[0:CLASSES, :] = cw[...].astype(F32)
        wct[:, 0:128] = cwf[0:32, :].astype(BF16)
        wct[:, 128:256] = cwf[0:32, :].astype(BF16)
        two[...] = jnp.zeros_like(two)
        two[0:32, 0:128] = cwf[0:32, :].astype(BF16)
        two[32:64, 128:256] = cwf[0:32, :].astype(BF16)
        cwf[...] = jnp.zeros_like(cwf)
        cwf[0:1, 0:CLASSES] = cb[...]
        bias[...] = jnp.broadcast_to(jnp.transpose(cwf[...])[0:24, 0:1], (24, 128))

    level3 = conv(3, x32, 0, fw.at[3], w32, y32, 64, p64)
    with scope("t_wait"):
        halo_wait("t0")
    with scope("l3"):
        run(level3, [((2, 3), (2, 3), 0)])
        moments(3, [2 * 64])
    copies["x8"].wait()
    halo_start("s1")
    halo_start("e")

    with scope("q_b"):
        late = run(quarter, band(11), late, keep=True)

    level2 = conv(2, x16, 0, fw.at[2], w16, y16, 128, p128)
    with scope("s_wait"):
        halo_wait("s0")
    with scope("l2"):
        level2[0](((1, 2), (1, 2), 0))
        level2[0](((3, 4), (3, 4), 1))

    with scope("q_c"):
        quarter[0](band(13)[0])
        for old in late:
            old()
        level2[1](((1, 2), (1, 2), 0))
        level2[1](((3, 4), (3, 4), 1))
        moments(2, [256, 256])
        halo_start("q", 0)
        edge_rows(((1, 2), (0, 1)), True)
        quarter[1](band(13)[0])
        quarter[1](((0, 15), (), 7))

    with scope("t12_wait"):
        halo_wait("t1")
        halo_wait("t2")
        copies["gain"].wait()
        copies["shift"].wait()
    with scope("l3_ext"):
        run(level3, [((0, 1, 4, 5), (), 1)])
    scale3 = scales(3, 2 * 64)
    level5 = conv(5, in5, 1, iw.at[1], wi.at[1], y5, 128, p128)
    with scope("l5"):
        normalize(y32, a32, scale3, 6, 1, 4)
        double(a32, u64, in5, [(k, 2 * k) for k in range(1, 5)], 4, 8)
        run(level5, [((2, 3),) * 2 + (0,), ((4, 5),) * 2 + (1,)])
        moments(5, [256, 256])
    halo_start("q", 1)
    halo_start("q", 2)
    level1 = conv(1, x8, 0, fw.at[1], w8, y8, 256, p256)
    level4 = conv(4, in4, 0, iw.at[0], wi.at[0], y4, 256, p256)
    inner = [((1, 2, 3, 4),) * 2 + (0,), ((5, 6),) * 2 + (1,), ((0, 7),) * 2 + (2,)]
    eight = [((0, 1, 2, 3),) * 2 + (0,), ((4, 5),) * 2 + (1,), ((6, 7),) * 2 + (2,)]
    with scope("l5_ext_l1"):
        double(a32, u64, in5, [(0, 0), (5, 10)], 4, 8)
        level5[0](((0, 1, 6, 7), (), 0))
        level1[0](inner[0])
        level5[1](((0, 1, 6, 7), (), 0))
        level1[0](inner[1])
        level1[1](inner[0])

    with scope("s1_wait"):
        halo_wait("s1")
        halo_start("q", 3)
    with scope("l2_ext"):
        level2[0](((0, 5), (), 0))
        level1[1](inner[1])
        level2[1](((0, 5), (), 0))
    with scope("e_wait"):
        halo_wait("e")
    with scope("l1_edge"):
        run(level1, inner[2:])
        moments(1, [1024, 512, 512])
    scale2 = scales(2, 4 * 128)
    with scope("l4"):
        normalize(y16, a16, scale2, 6, 0, 5)
        double(a16, u128, in4, [(k, 2 * k - 1) for k in range(4)], 1, 9)
        level4[0](eight[0])
        double(a16, u128, in4, [(k, 2 * k - 1) for k in range(4, 6)], 1, 9)
        level4[0](eight[1])
        level4[1](eight[0])
        level4[0](eight[2])
        level4[1](eight[1])
        level4[1](eight[2])
        moments(4, [1024, 512, 512])

    scale5 = scales(5, 4 * 128)
    level6 = conv(6, in6, 0, iw.at[2], wi.at[2], y6, 256, p256)
    with scope("l6"):
        normalize(y5, a5, scale5, 8, 1, 6)
        double(a5, u128, in6, [(k, 2 * k - 2) for k in range(1, 5)], 2, 10)
        own = [((1, 2, 3, 4),) * 2 + (0,), ((5, 6),) * 2 + (1,), ((7, 8),) * 2 + (2,)]
        level6[0](own[0])
        double(a5, u128, in6, [(k, 2 * k - 2) for k in range(5, 7)], 2, 10)
        level6[0](own[1])
        level6[1](own[0])
        level6[0](own[2])
        level6[1](own[1])
        level6[1](own[2])
        moments(6, [1024, 512, 512])

    with scope("q_wait_e"):
        halo_wait("q")
    with scope("q_e"):
        edge_rows(((0,), (2,)), False)
        quarter[1](((0, 15), (0, 15), 7))
        moments(0, [1024] * 8)
        copies["lab"].wait()

    with scope("l6_ext"):
        run(level6, [((0, 9), (), 1)])
    scale1 = scales(1, 8 * 256)
    scale4 = scales(4, 8 * 256)
    with scope("z14"):
        for half in range(2):
            act = jnp.concatenate(
                [jnp.concatenate([activate(y4[r], scale4), activate(y8[r], scale1)], axis=1)
                 for r in range(half * 4, half * 4 + 4)], axis=0)
            part = lax.dot_general(wct[...], act, nt, preferred_element_type=F32)
            for i in range(4):
                zt[half * 4 + i] = part[0:24, i * 256 : (i + 1) * 256]
    halo_start("z")
    scale6 = scales(6, 8 * 256)
    with scope("z6"):
        act = jnp.concatenate(
            [jnp.concatenate([activate(y6[r], scale6), activate(y6[r + 1], scale6)], axis=1)
             for r in range(0, 10, 2)], axis=0)
        part = lax.dot_general(two[...], act, nt, preferred_element_type=F32)
        for r in range(10):
            z6[r] = part[r % 2 * 32 : r % 2 * 32 + 24, r // 2 * 256 : r // 2 * 256 + 256]

    def widen(flat):
        high = flat.astype(BF16)
        low = (flat - high.astype(F32)).astype(BF16)
        return (jnp.dot(high, u256[...], preferred_element_type=F32)
                + jnp.dot(low, u256[...], preferred_element_type=F32))

    with scope("widen"):
        zc[1:9] = widen((zt[...] + z6[1:9]).reshape(192, 256)).reshape(8, 24, 512)

        @pl.when(pos == 0)
        def _():
            ze[0] = zt[0]
            z6[0] = z6[1]

        @pl.when(pos == last)
        def _():
            ze[1] = zt[7]
            z6[9] = z6[8]

    scale0 = scales(0, 16 * 512)

    def finish(rows):
        act = jnp.concatenate([activate(yq[r], scale0) for r in rows], axis=1)
        main = lax.dot_general(two[...], act, nt, preferred_element_type=F32)
        kind = lax.broadcasted_iota(jnp.int32, (24, 512), 0)
        offset = jnp.concatenate([bias[...]] * 4, axis=1)
        for i, r in enumerate(rows):
            half = r // 2
            near = half + 2 * (r % 2)
            score = (main[i * 32 : i * 32 + 24] + offset
                     + 0.75 * zc[half + 1] + 0.25 * zc[near])
            grown = jnp.where(kind < CLASSES, jnp.exp(score), 0.0)
            sums[r : r + 1, :] = jnp.sum(grown, axis=0, keepdims=True)
            marks = jnp.broadcast_to(lab[r : r + 1, :], (24, 512))
            picks[r : r + 1, :] = jnp.sum(
                jnp.where(kind == marks, score, 0.0), axis=0, keepdims=True)
            for block in range(4):
                tall[block, r * 36 : r * 36 + 24, :] = score[:, block * 128 : (block + 1) * 128]

    with scope("finish"):
        for r in range(1, 15, 2):
            finish((r, r + 1))
    with scope("z_wait"):
        halo_wait("z")
    with scope("finish_edge"):
        edges = widen(jnp.concatenate([ze[0] + z6[0], ze[1] + z6[9]], axis=0))
        zc[0] = edges[0:24]
        zc[9] = edges[24:48]
        finish((0, 15))

    with scope("loss_terms"):
        usable = lab[...] != 255
        terms = jnp.where(usable, jnp.log(sums[...]) - picks[...], 0.0)
        both = []
        for part in (terms, usable.astype(F32)):
            part = jnp.sum(part, axis=0, keepdims=True)
            both.append(part[:, 0:128] + part[:, 128:256] + part[:, 256:384] + part[:, 384:512])
        sub = lax.broadcasted_iota(jnp.int32, (8, 128), 0)
        loss_rows[pos] = jnp.where(
            sub == 0, jnp.broadcast_to(both[0], (8, 128)), jnp.broadcast_to(both[1], (8, 128)))[0:2]

    def loss_copy(ref, slot, index, target):
        return pltpu.make_async_remote_copy(
            src_ref=ref.at[slot], dst_ref=ref.at[slot],
            send_sem=loss_send.at[index], recv_sem=loss_recv.at[index],
            device_id=target, device_id_type=MESH,
        )

    for peer in row_peers():
        loss_copy(loss_rows, pos, 0, {"rows": peer}).start()

    with scope("scores_out"):
        for k in range(CLASSES):
            for block in range(4):
                out_ref[0, k, :, block * 128 : (block + 1) * 128] = tall[
                    block, pl.ds(k, 16, stride=36), :
                ].astype(BF16)

    with scope("loss_wait_rows"):
        tiles_wait(loss_rows.at[pl.ds(0, nr - 1)], loss_recv.at[0])
    loss_batch[bat] = functools.reduce(lambda a, b: a + b, [loss_rows[i] for i in range(nr)])

    for peer in batch_peers():
        loss_copy(loss_batch, bat, 1, {"batch": peer}).start()

    with scope("sent_waits"):
        for name in ("t0", "t1", "t2", "s0", "s1", "e", "q", "z"):
            halo_sent(name)
        for layer in range(7):
            tiles_wait(stats.at[layer, pl.ds(0, nr - 1)], stat_send.at[layer])
        tiles_wait(loss_rows.at[pl.ds(0, nr - 1)], loss_send.at[0])
    with scope("loss_wait_batch"):
        tiles_wait(loss_batch.at[pl.ds(0, nb - 1)], loss_recv.at[1])
    whole = functools.reduce(lambda a, b: a + b, [loss_batch[i] for i in range(nb)])
    whole = jnp.broadcast_to(jnp.sum(whole, axis=1, keepdims=True), (2, 128))
    loss_ref[...] = whole[0:1] / jnp.maximum(whole[1:2], 1.0)
    tiles_wait(loss_batch.at[pl.ds(0, nb - 1)], loss_send.at[1])


def solution(mesh):
    nb, nr = mesh.shape["batch"], mesh.shape["rows"]

    def per_device(xq, x8, x16, x32, labels, fw, iw, gain, shift, cw, cb):
        any_spec = pl.BlockSpec(memory_space=pl.ANY)
        vmem = pl.BlockSpec(memory_space=pltpu.VMEM)
        V = pltpu.VMEM
        dma = pltpu.SemaphoreType.DMA
        logits, loss = pl.pallas_call(
            functools.partial(kernel, nb, nr),
            out_shape=(
                V((1, CLASSES, 16, 512), BF16),
                V((1, 128), F32),
            ),
            in_specs=[any_spec] * 11,
            out_specs=(vmem, vmem),
            scratch_shapes=[
                V((18, 512, 256), BF16), V((10, 256, 256), BF16), V((8, 128, 256), BF16),
                V((8, 64, 256), BF16), V((16, 512), jnp.int32), V((4, 3, 3, 256, 128), BF16),
                V((3, 3, 3, 128, 128), BF16), V((7, 128), F32), V((7, 128), F32),
                V((CLASSES, 128), BF16), V((1, CLASSES), F32),
                V((16, 512, 128), F32), V((8, 256, 128), F32), V((6, 128, 128), F32),
                V((6, 64, 128), F32), V((8, 256, 128), F32), V((8, 128, 128), F32),
                V((10, 256, 128), F32),
                V((6, 128, 128), BF16), V((6, 64, 128), BF16), V((8, 128, 128), BF16),
                V((10, 256, 128), BF16), V((12, 128, 128), BF16), V((12, 256, 128), BF16),
                V((2, 2, 2, 528, 128), F32), V((2, 2, 4, 272, 128), F32),
                V((2, 2, 6, 144, 128), F32), V((2, 2, 6, 80, 128), F32),
                V((128, 128), F32), V((256, 256), BF16), V((256, 512), BF16),
                V((128, 128), F32), V((32, 256), BF16), V((64, 256), BF16), V((24, 128), F32),
                V((8, 24, 256), F32), V((2, 24, 256), F32), V((10, 24, 256), F32),
                V((10, 24, 512), F32),
                V((16, 512), F32), V((16, 512), F32), V((4, 16 * 36, 128), F32),
                V((1024, 256), BF16), V((1024, 256), BF16), V((1024, 256), BF16),
                V((1024, 256), BF16), V((3, 512, 256), BF16),
                V((7, 8, 8, 128), F32), V((7, nr, 2, 128), F32), V((nr, 2, 128), F32),
                V((nb, 2, 128), F32),
                dma((15,)), dma((16,)), dma((16,)), dma((7,)), dma((7,)), dma((2,)), dma((2,)),
            ],
            compiler_params=pltpu.CompilerParams(
                collective_id=0, has_side_effects=True, vmem_limit_bytes=60 * 1024 * 1024
            ),
        )(xq, x8, x16, x32, labels, fw, iw, gain, shift, cw.T, cb.reshape(1, CLASSES))
        return logits, loss[0, 0]

    batch, rows = "batch", "rows"
    return jax.shard_map(
        per_device, mesh=mesh,
        in_specs=(P(batch, rows, None, None),) * 4 + (P(batch, rows, None),) + (P(),) * 6,
        out_specs=(P(batch, None, rows, None), P()),
        check_vma=False,
    )
```
